512 devices in a mesh: lon: 128 (over x_lo, z, y), lat: 4 (over x_hi, core).
Axes of the slice: x: 4 (x_hi: 2, x_lo: 2; x = x_hi * 2 + x_lo), y: 8, z: 8, core: 2. Of those that a mesh axis runs over, the one named last changes fastest.
Arguments:
- inverse: float32 [256, 8, 128, 128], P('lon', 'lat'), may hold values from -0.1 to 0.2
- vert_diag: float32 [256, 8, 128], P('lon', 'lat'), may hold values from 0.1 to 1
- vert_coup: float32 [256, 8, 128], P('lon', 'lat'), may hold values from 0.5 to 4
- face_east: float32 [256, 8, 128], P('lon', 'lat'), may hold values from 0.3 to 3
- face_north: float32 [256, 8, 128], P('lon', 'lat'), may hold values from 0.3 to 3
- land_mask: int32 [256, 8], P('lon', 'lat'), may hold values 0 or 1
- aggregate: int32 [256, 8], P('lon', 'lat'), may hold values from -1 to 511, as said below
Outputs:
- coarse: float32 [128, 4, 13, 128, 128], P('lon', 'lat')
The draws below stay inside these ranges and needn't reach their ends.
Inputs may be any that keep to these rules, and one draw needn't show every extreme that they name: `aggregate`: each entry is -1 (the column belongs to no coarse column) or the index I * 4 + J of the coarse column (I, J) = (i // 2, j // 2) of its own 2 x 2 block; -1 may occur anywhere and is more frequent in the two fine latitudes nearest each end of the latitude range.
All inputs are finite; a program needn't handle non-finite values. No bound on the sum of `land_mask` on one device may be relied on, other than what follows from the above.
Results may differ from the reference program's by a relative error of at most 0.0002.
Values sent between devices are 32-bit elements; how exact they have to be, the bound alone decides.
A program may use at most 64 MiB of HBM per device.

```python
import math
import jax
import jax.numpy as jnp
from jax import lax

NZ = 128
NX = 256
NY = 8
NXC = 128
NYC = 4


def draw_inverse(key, part):
    diag_key, entry_key = jax.random.split(jax.random.fold_in(key, 11), 2)
    diagonal = jnp.exp(jax.random.uniform(diag_key, (NX, NY, NZ), jnp.float32, math.log(0.05), math.log(0.2)))
    spread = 0.05 / math.sqrt(NZ)
    entries = jax.random.truncated_normal(entry_key, -4.0, 4.0, (NX, NY, NZ, NZ), jnp.float32) * spread
    identity = jnp.eye(NZ, dtype=jnp.float32)
    return (entries * (1.0 - identity) + diagonal[..., None] * identity).astype(jnp.float32)


def draw_aggregate(key, part):
    lon_index = lax.broadcasted_iota(jnp.int32, (NX, NY), 0)
    lat_index = lax.broadcasted_iota(jnp.int32, (NX, NY), 1)
    natural = lon_index // 2 * NYC + lat_index // 2
    polar = (lat_index < 2) | (lat_index >= NY - 2)
    rolled = jax.random.randint(jax.random.fold_in(key, 23), (NX, NY), 0, 8)
    dropped = jnp.where(polar, rolled < 4, rolled < 1)
    return jnp.where(dropped, -1, natural).astype(jnp.int32)


def set_ends(drawn, rng, least, high):
    extent = drawn.shape
    index_at = [jax.random.randint(jax.random.fold_in(rng, axis), (), 0, extent[axis]) for axis in range(len(extent))]
    drawn = drawn.at[tuple(index_at)].set(least)
    longest = extent.index(max(extent))
    index_at[longest] = (index_at[longest] + 1) % extent[longest]
    return drawn.at[tuple(index_at)].set(high)


def level_of(own_key, extent, cuts, low, high):
    level = 1.0
    for axis_at, parts in cuts:
        heights = jax.random.uniform(jax.random.fold_in(jax.random.fold_in(own_key, 6), axis_at), (parts,), jnp.float32, low / len(cuts), high / len(cuts))
        level = level * jnp.repeat(jnp.exp(heights), extent[axis_at] // parts).reshape((-1,) + (1,) * (len(extent) - 1 - axis_at))
    return level


def setup_inputs(seed: int = 0) -> dict:
    streams_of = jax.random.split(jax.random.key(seed), 8)
    inverse = draw_inverse(jax.random.fold_in(streams_of[7], 71), 0)
    vert_diag = jnp.clip(jnp.exp(math.log(1.0) - 2.3025851 * jax.random.uniform(streams_of[1], (NX, NY, NZ), jnp.float32) ** level_of(streams_of[1], (NX, NY, NZ), ((0, 128), (1, 4)), -0.2, 0.2)), 0.1, 1.0)
    vert_coup = jnp.clip(jnp.exp(math.log(4.0) - 2.0794415 * jax.random.uniform(streams_of[2], (NX, NY, NZ), jnp.float32) ** level_of(streams_of[2], (NX, NY, NZ), ((0, 128), (1, 4)), -0.2, 0.2)), 0.5, 4.0)
    face_east = jnp.clip(jnp.exp(math.log(3.0) - 2.3025851 * jax.random.uniform(streams_of[3], (NX, NY, NZ), jnp.float32) ** level_of(streams_of[3], (NX, NY, NZ), ((0, 128), (1, 4)), -0.2, 0.2)), 0.3, 3.0)
    face_north = jnp.clip(jnp.exp(math.log(3.0) - 2.3025851 * jax.random.uniform(streams_of[4], (NX, NY, NZ), jnp.float32) ** level_of(streams_of[4], (NX, NY, NZ), ((0, 128), (1, 4)), -0.2, 0.2)), 0.3, 3.0)
    land_mask = set_ends((jax.random.randint(streams_of[5], (NX, NY), 0, 8) < 7).astype(jnp.int32), jax.random.fold_in(streams_of[5], 1), 0, 1)
    aggregate = draw_aggregate(jax.random.fold_in(streams_of[7], 71), 0)
    return dict(inverse=inverse, vert_diag=vert_diag, vert_coup=vert_coup, face_east=face_east, face_north=face_north, land_mask=land_mask, aggregate=aggregate)


relax_weight = 0.6
stencil_offsets = [(-2, 0), (-1, -1), (-1, 0), (-1, 1), (0, -2), (0, -1), (0, 0), (0, 1), (0, 2), (1, -1), (1, 0), (1, 1), (2, 0)]

def shift_levels_down(values):
    return jnp.concatenate([jnp.zeros_like(values[..., :1]), values[..., :-1]], axis=-1)

def shift_levels_up(values):
    return jnp.concatenate([values[..., 1:], jnp.zeros_like(values[..., :1])], axis=-1)

def shift_rows_down(blocks):
    return jnp.concatenate([jnp.zeros_like(blocks[..., :1, :]), blocks[..., :-1, :]], axis=-2)

def shift_rows_up(blocks):
    return jnp.concatenate([blocks[..., 1:, :], jnp.zeros_like(blocks[..., :1, :])], axis=-2)

def block_steps(parity_lon, parity_lat):
    lon_step = -1 if parity_lon == 0 else 1
    lat_step = -1 if parity_lat == 0 else 1
    return [(0, 0), (lon_step, 0), (0, lat_step)]

def off_coupling(vertical):
    levels = vertical.shape[-1]
    level_index = lax.broadcasted_iota(jnp.int32, vertical.shape, vertical.ndim - 1)
    return jnp.where(level_index < levels - 1, vertical, jnp.zeros_like(vertical))

def prolong_rows(inverse_block, column_data, parity_lon, parity_lat):
    main_diag = column_data[..., 0, :]
    coupling = off_coupling(column_data[..., 1, :])
    east_weighted = column_data[..., 2, :]
    west_weighted = column_data[..., 3, :]
    north_weighted = column_data[..., 4, :]
    south_weighted = column_data[..., 5, :]
    weights = column_data[..., 8, :]
    same_lon = east_weighted if parity_lon == 0 else west_weighted
    cross_lon = west_weighted if parity_lon == 0 else east_weighted
    same_lat = north_weighted if parity_lat == 0 else south_weighted
    cross_lat = south_weighted if parity_lat == 0 else north_weighted
    diagonal_part = weights * main_diag - same_lon - same_lat
    coupling_below = shift_levels_down(coupling)
    left_cols = shift_levels_down(inverse_block)
    right_cols = shift_levels_up(inverse_block)
    smoothed = inverse_block * diagonal_part[..., None, :] - weights[..., None, :] * (left_cols * coupling_below[..., None, :] + right_cols * coupling[..., None, :])
    levels = inverse_block.shape[-1]
    identity = (lax.broadcasted_iota(jnp.int32, (levels, levels), 0) == lax.broadcasted_iota(jnp.int32, (levels, levels), 1)).astype(jnp.float32)
    own_block = weights[..., None, :] * identity - relax_weight * smoothed
    lon_block = relax_weight * inverse_block * cross_lon[..., None, :]
    lat_block = relax_weight * inverse_block * cross_lat[..., None, :]
    return jnp.stack([own_block, lon_block, lat_block], axis=-3)

def apply_column(column_data, blocks):
    main_diag = column_data[..., 0, :]
    coupling = off_coupling(column_data[..., 1, :])
    coupling_below = shift_levels_down(coupling)
    return main_diag[..., None, :, None] * blocks - coupling_below[..., None, :, None] * shift_rows_down(blocks) - coupling[..., None, :, None] * shift_rows_up(blocks)

def contract(left, right):
    return jnp.einsum('xyrk,xyrl->xykl', left, right, precision=lax.Precision.HIGHEST, preferred_element_type=jnp.float32)

def reference(inverse, vert_diag, vert_coup, face_east, face_north, land_mask, aggregate):
    live_cols = (aggregate >= 0).astype(jnp.float32)
    block_count = live_cols.reshape(NXC, 2, NYC, 2).sum(axis=(1, 3))
    block_count = jnp.repeat(jnp.repeat(block_count, 2, axis=0), 2, axis=1)
    weights = live_cols / jnp.sqrt(jnp.maximum(block_count, 1.0))
    land_open = land_mask.astype(jnp.float32)
    lat_index = lax.broadcasted_iota(jnp.int32, (NX, NY), 1)
    east_open = land_open * jnp.roll(land_open, -1, axis=0)
    north_open = land_open * jnp.roll(land_open, -1, axis=1) * (lat_index < NY - 1).astype(jnp.float32)
    east_face = face_east * east_open[:, :, None]
    north_face = face_north * north_open[:, :, None]
    west_face = jnp.roll(east_face, 1, axis=0)
    south_face = jnp.roll(north_face, 1, axis=1)
    weight_col = jnp.broadcast_to(weights[:, :, None], vert_diag.shape)
    east_weighted = east_face * jnp.roll(weight_col, -1, axis=0)
    west_weighted = west_face * jnp.roll(weight_col, 1, axis=0)
    north_weighted = north_face * jnp.roll(weight_col, -1, axis=1)
    south_weighted = south_face * jnp.roll(weight_col, 1, axis=1)
    main_diag = vert_diag + vert_coup + shift_levels_down(vert_coup) + east_face + west_face + north_face + south_face
    column_data = jnp.stack([main_diag, vert_coup, east_weighted, west_weighted, north_weighted, south_weighted, east_face, north_face, weight_col], axis=2)
    inverse_split = inverse.reshape(NXC, 2, NYC, 2, NZ, NZ)
    data_split = column_data.reshape(NXC, 2, NYC, 2, 9, NZ)
    classes = {}
    data_classes = {}
    for parity_lon in (0, 1):
        for parity_lat in (0, 1):
            class_data = data_split[:, parity_lon, :, parity_lat]
            data_classes[parity_lon, parity_lat] = class_data
            classes[parity_lon, parity_lat] = prolong_rows(inverse_split[:, parity_lon, :, parity_lat], class_data, parity_lon, parity_lat)
    offset_slot = {offset: place for place, offset in enumerate(stencil_offsets)}
    slots = [jnp.zeros((NXC, NYC, NZ, NZ), jnp.float32) for offset in stencil_offsets]

    def add_term(landing, target, term):
        place = offset_slot[target[0] - landing[0], target[1] - landing[1]]
        slots[place] = slots[place] + jnp.roll(term, landing, axis=(0, 1))
    for parity_lon in (0, 1):
        for parity_lat in (0, 1):
            own_rows = classes[parity_lon, parity_lat]
            own_data = data_classes[parity_lon, parity_lat]
            own_applied = apply_column(own_data, own_rows)
            own_steps = block_steps(parity_lon, parity_lat)
            for left_index in range(3):
                for right_index in range(left_index, 3):
                    term = contract(own_rows[:, :, left_index], own_applied[:, :, right_index])
                    add_term(own_steps[left_index], own_steps[right_index], term)
                    if right_index != left_index:
                        add_term(own_steps[right_index], own_steps[left_index], jnp.swapaxes(term, -1, -2))
            for face_dir in (0, 1):
                if face_dir == 0:
                    partner_key = (1 - parity_lon, parity_lat)
                    shift = (parity_lon, 0)
                    face = own_data[:, :, 6]
                else:
                    partner_key = (parity_lon, 1 - parity_lat)
                    shift = (0, parity_lat)
                    face = own_data[:, :, 7]
                partner_rows = classes[partner_key]
                if shift[0] == 1:
                    partner_rows = jnp.roll(partner_rows, -1, axis=0)
                if shift[1] == 1:
                    partner_rows = jnp.roll(partner_rows, -1, axis=1)
                partner_steps = block_steps(partner_key[0], partner_key[1])
                for left_index in range(3):
                    for right_index in range(3):
                        target = (shift[0] + partner_steps[right_index][0], shift[1] + partner_steps[right_index][1])
                        term = -contract(own_rows[:, :, left_index], face[:, :, :, None] * partner_rows[:, :, right_index])
                        add_term(own_steps[left_index], target, term)
                        add_term(target, own_steps[left_index], jnp.swapaxes(term, -1, -2))
    return jnp.stack(slots, axis=2)
```

```python
import jax
import jax.numpy as jnp
from jax import lax
from jax.experimental import pallas as pl
from jax.experimental.pallas import tpu as pltpu
from jax.sharding import PartitionSpec as P

MESH = pl.DeviceIdType.MESH
relax = 0.6
offsets = [
    (-2, 0),
    (-1, -1),
    (-1, 0),
    (-1, 1),
    (0, -2),
    (0, -1),
    (0, 0),
    (0, 1),
    (0, 2),
    (1, -1),
    (1, 0),
    (1, 1),
    (2, 0),
]
slot_of = {offset: place for place, offset in enumerate(offsets)}
near_blocks = [(0, 0), (1, 0), (-1, 0), (0, 1), (0, -1)]
second_blocks = [(2, 0), (-2, 0), (0, 2), (0, -2)]
corner_blocks = [(1, 1), (-1, 1), (1, -1), (-1, -1)]
sides = [(1, 0), (-1, 0), (0, 1), (0, -1)]


def corner_cell(block):
    return (0 if block[0] > 0 else 1, 0 if block[1] > 0 else 1)


def cells_of(block):
    return [(2 * block[0] + p, 2 * block[1] + r) for p in (0, 1) for r in (0, 1)]


def near_cells(side):
    a, b = side
    if b == 0:
        p = 0 if a > 0 else 1
        return [(2 * a + p, r) for r in (0, 1)]
    r = 0 if b > 0 else 1
    return [(p, 2 * b + r) for p in (0, 1)]


def far_cells(side):
    near = near_cells(side)
    return [cell for cell in cells_of(side) if cell not in near]


def neighbours(cell):
    x, y = cell
    return [(x + 1, y), (x - 1, y), (x, y + 1), (x, y - 1)]


own_cells = cells_of((0, 0))
support = own_cells + [cell for side in sides for cell in near_cells(side)]
outer = [cell for side in sides for cell in far_cells(side)] + [
    (2 * a + corner_cell((a, b))[0], 2 * b + corner_cell((a, b))[1]) for a, b in corner_blocks
]
all_cells = support + outer
cell_index = {cell: place for place, cell in enumerate(all_cells)}
COEFS = 9
edge_list = []
for cell in support:
    for other in neighbours(cell):
        key = tuple(sorted((cell, other)))
        if key not in edge_list:
            edge_list.append(key)
edge_index = {edge: COEFS * len(all_cells) + place for place, edge in enumerate(edge_list)}
coef_rows = COEFS * len(all_cells) + len(edge_list)
coef_rows = (coef_rows + 7) // 8 * 8

message = {}
for block in near_blocks[1:] + second_blocks + corner_blocks:
    message["packet", block] = len(message)
for side in sides:
    for cell in near_cells(side) + far_cells(side):
        message["block", cell] = len(message)
for block in corner_blocks:
    message["corner", block] = len(message)


def down(values):
    lane = lax.broadcasted_iota(jnp.int32, values.shape, 1)
    return jnp.where(lane > 0, pltpu.roll(values, 1, 1), 0.0)


def split(values):
    high = values.astype(jnp.bfloat16)
    low = (values - high.astype(jnp.float32)).astype(jnp.bfloat16)
    return high, low


def kernel(
    inv_h, vd_h, vc_h, fe_h, fn_h, land_h, agg_h,
    out,
    X, XC, PK, PC, PD, SD, SM, LA, PT, CF,
    local_sem, send_sem, recv_sem,
):
    me_lon = lax.axis_index("lon")
    me_lat = lax.axis_index("lat")
    count_lon = lax.axis_size("lon")
    count_lat = lax.axis_size("lat")
    own_of = {"vd": 0, "vc": 1, "fe": 2, "fn": 3}

    inverse_copy = pltpu.make_async_copy(inv_h, X.at[0], local_sem.at[0])
    small_copies = [
        pltpu.make_async_copy(source, SM.at[place], local_sem.at[1 + place])
        for place, source in enumerate((vd_h, vc_h, fe_h, fn_h))
    ] + [
        pltpu.make_async_copy(source, LA.at[place], local_sem.at[5 + place])
        for place, source in enumerate((land_h, agg_h))
    ]
    for copy in small_copies:
        copy.start()
    inverse_copy.start()

    def target(block):
        a, b = block
        return {"lon": lax.rem(me_lon + a + count_lon, count_lon), "lat": me_lat + b}

    def exists(block):
        b = block[1]
        if b == 0:
            return None
        return me_lat + b < count_lat if b > 0 else me_lat + b >= 0

    def only(condition, action):
        if condition is None:
            action()
        else:
            pl.when(condition)(action)

    partners = near_blocks[1:] + second_blocks + corner_blocks
    barrier = pltpu.get_barrier_semaphore()
    for block in partners:
        def signal(block=block):
            pl.semaphore_signal(barrier, inc=1, device_id=target(block), device_id_type=MESH)
        only(exists(block), signal)

    for block in partners:
        if block[1] == 0:
            continue
        def clear(block=block):
            if block in near_blocks:
                place = near_blocks.index(block)
                PK[place] = jnp.zeros((24, 128), jnp.float32)
                X[place] = jnp.zeros((2, 2, 128, 128), jnp.float32)
            elif block in second_blocks:
                PC[second_blocks.index(block)] = jnp.zeros((8, 128), jnp.float32)
            else:
                PD[corner_blocks.index(block)] = jnp.zeros((8, 128), jnp.float32)
                XC[corner_blocks.index(block)] = jnp.zeros((128, 128), jnp.float32)
        pl.when(jnp.logical_not(exists(block)))(clear)

    for copy in small_copies:
        copy.wait()
    live = (LA[1] >= 0).astype(jnp.float32)
    land = LA[0].astype(jnp.float32)

    def spread(values, p, r):
        return jnp.broadcast_to(values[p : p + 1, r : r + 1], (1, 128))

    lives = {(p, r): spread(live, p, r) for p in (0, 1) for r in (0, 1)}
    block_count = lives[0, 0] + lives[0, 1] + lives[1, 0] + lives[1, 1]
    norm = jnp.sqrt(jnp.maximum(block_count, 1.0))
    lane = lax.broadcasted_iota(jnp.int32, (1, 128), 1)
    scalars = jnp.zeros((1, 128), jnp.float32)
    for p in (0, 1):
        for r in (0, 1):
            scalars = jnp.where(lane == 2 * p + r, spread(land, p, r), scalars)
            scalars = jnp.where(lane == 4 + 2 * p + r, lives[p, r] / norm, scalars)

    def mine(field, p, r):
        return SM[own_of[field], p, pl.ds(r, 1), :]

    blank = jnp.zeros((1, 128), jnp.float32)
    head = [scalars, mine("fe", 1, 0), mine("fe", 1, 1), mine("fn", 0, 1), mine("fn", 1, 1)]
    for row, values in enumerate(head + [blank] * 3):
        PK[0, pl.ds(row, 1), :] = values
    for first, field in ((8, "fe"), (12, "fn"), (16, "vd"), (20, "vc")):
        for p in (0, 1):
            for r in (0, 1):
                PK[0, pl.ds(first + 2 * p + r, 1), :] = mine(field, p, r)
    lands = {(p, r): spread(land, p, r) for p in (0, 1) for r in (0, 1)}
    for place, block in enumerate(corner_blocks):
        p, r = corner_cell(block)
        east = mine("fe", 0, r) * (lands[0, r] * lands[1, r])
        north = mine("fn", p, 0) * (lands[p, 0] * lands[p, 1])
        vc = mine("vc", p, r)
        inner = lives[p, r] / norm * (mine("vd", p, r) + vc + down(vc) + east + north)
        inner = inner - (east * (lives[1 - p, r] / norm) + north * (lives[p, 1 - r] / norm))
        for row, values in enumerate(head + [inner, vc, blank]):
            SD[place, pl.ds(row, 1), :] = values

    lat_near = jnp.where(me_lat + 1 < count_lat, 3, 0) + jnp.where(me_lat >= 1, 3, 0)
    lat_second = jnp.where(me_lat + 2 < count_lat, 1, 0) + jnp.where(me_lat >= 2, 1, 0)
    pl.semaphore_wait(barrier, 4 + lat_near + lat_second)

    def move(key, source, landing, block):
        place = message[key]
        return pltpu.make_async_remote_copy(
            src_ref=source,
            dst_ref=landing,
            send_sem=send_sem.at[place],
            recv_sem=recv_sem.at[place],
            device_id=target(block),
            device_id_type=MESH,
        )

    def opposite(block):
        return (-block[0], -block[1])

    sends = []

    def send(key, source, landing, block, condition):
        copy = move(key, source, landing, block)
        only(condition, copy.start)
        sends.append((copy, condition))

    def packet_landing(block):
        if block in near_blocks:
            return PK.at[near_blocks.index(block)]
        if block in second_blocks:
            return PC.at[second_blocks.index(block)]
        return PD.at[corner_blocks.index(block)]

    def packet_source(block):
        if block in near_blocks:
            return PK.at[0]
        if block in second_blocks:
            return PK.at[0, pl.ds(0, 8)]
        return SD.at[corner_blocks.index(block)]

    for block in partners:
        goal = opposite(block)
        send(("packet", block), packet_source(block), packet_landing(block), goal, exists(goal))

    def block_ref(cell):
        x, y = cell
        block = (x // 2, y // 2)
        if block in near_blocks:
            return X.at[near_blocks.index(block), x % 2, y % 2]
        return XC.at[corner_blocks.index(block)]

    def block_value(cell):
        x, y = cell
        block = (x // 2, y // 2)
        if block in near_blocks:
            return X[near_blocks.index(block), x % 2, y % 2]
        return XC[corner_blocks.index(block)]

    inverse_copy.wait()
    for cells in (near_cells, far_cells):
        for step in (0, 1):
            for side in sides:
                cell = cells(side)[step]
                goal = opposite(side)
                source = X.at[0, cell[0] % 2, cell[1] % 2]
                send(("block", cell), source, block_ref(cell), goal, exists(goal))

    def wait_packet(block):
        copy = move(("packet", block), packet_source(block), packet_landing(block), block)
        only(exists(block), copy.wait_recv)

    def wait_block(cell):
        block = (cell[0] // 2, cell[1] // 2)
        copy = move(("block", cell), X.at[0, 0, 0], block_ref(cell), block)
        only(exists(block), copy.wait_recv)

    cache = {}

    def field(name, cell):
        if (name, cell) in cache:
            return cache[name, cell]
        x, y = cell
        block = (x // 2, y // 2)
        p, r = x % 2, y % 2
        place = 2 * p + r
        if block in near_blocks:
            ref, at = PK, near_blocks.index(block)
            row = {"fe": 8, "fn": 12, "vd": 16, "vc": 20}.get(name, 0) + place
        else:
            if block in second_blocks:
                ref, at = PC, second_blocks.index(block)
            else:
                ref, at = PD, corner_blocks.index(block)
            if name == "fe":
                assert p == 1
                row = 1 + r
            elif name == "fn":
                assert r == 1
                row = 3 + p
            elif name in ("inner", "vc"):
                assert (p, r) == corner_cell(block)
                row = 5 if name == "inner" else 6
        if name in ("land", "w"):
            lane_at = place + (4 if name == "w" else 0)
            row_values = ref[at, pl.ds(0, 1), :]
            value = jnp.broadcast_to(row_values[:, lane_at : lane_at + 1], (1, 128))
        else:
            value = ref[at, pl.ds(row, 1), :]
        cache[name, cell] = value
        return value

    def face(low, high):
        if ("face", low, high) not in cache:
            name = "fe" if low[1] == high[1] else "fn"
            cache["face", low, high] = field(name, low) * (field("land", low) * field("land", high))
        return cache["face", low, high]

    def between(cell, other):
        return face(*sorted((cell, other)))

    def coef(cell, row):
        return CF[pl.ds(COEFS * cell_index[cell] + row, 1), :]

    def edge(cell, other):
        return CF[pl.ds(edge_index[tuple(sorted((cell, other)))], 1), :]

    top = lax.broadcasted_iota(jnp.int32, (1, 128), 1) < 127

    def make_coefs(cell):
        x, y = cell
        p, r = x % 2, y % 2
        lon_cross, lon_same = ((x - 1, y), (x + 1, y)) if p == 0 else ((x + 1, y), (x - 1, y))
        lat_cross, lat_same = ((x, y - 1), (x, y + 1)) if r == 0 else ((x, y + 1), (x, y - 1))
        w = field("w", cell)
        vc = field("vc", cell)
        if abs(x // 2) + abs(y // 2) == 2 and x // 2 and y // 2:
            crossing = between(cell, lon_cross) + between(cell, lat_cross)
            weighted = field("inner", cell) + w * crossing
        else:
            main = field("vd", cell) + vc + down(vc)
            for other in neighbours(cell):
                main = main + between(cell, other)
            same = between(cell, lon_same) * field("w", lon_same)
            same = same + between(cell, lat_same) * field("w", lat_same)
            weighted = w * main - same
        up = jnp.where(top, vc, 0.0)
        below = down(up)
        rows = [
            w,
            -relax * weighted,
            relax * w * below,
            relax * w * up,
            relax * between(cell, lon_cross) * field("w", lon_cross),
            relax * between(cell, lat_cross) * field("w", lat_cross),
        ]
        if cell in support:
            rows += [main, -below, -up]
        for row, values in enumerate(rows):
            CF[pl.ds(COEFS * cell_index[cell] + row, 1), :] = values

    for block in near_blocks[1:]:
        wait_packet(block)
    for cell in own_cells:
        make_coefs(cell)

    def roll_down(values):
        return pltpu.roll(values, 1, 1)

    def roll_up(values):
        return pltpu.roll(values, 127, 1)

    diagonal = lax.broadcasted_iota(jnp.int32, (128, 128), 0) == lax.broadcasted_iota(
        jnp.int32, (128, 128), 1
    )
    for cell in own_cells:
        inverse = block_value(cell)
        values = jnp.where(diagonal, coef(cell, 0), 0.0) + inverse * coef(cell, 1)
        values = values + roll_down(inverse) * coef(cell, 2) + roll_up(inverse) * coef(cell, 3)
        PT[cell_index[cell]] = values.T

    for block in second_blocks + corner_blocks:
        wait_packet(block)
    for cell in all_cells:
        if cell not in own_cells:
            make_coefs(cell)
    for low, high in edge_list:
        CF[pl.ds(edge_index[low, high], 1), :] = face(low, high)

    def relay(condition, source_cell, corner, goal):
        def start():
            move(("corner", corner), block_ref(source_cell), XC.at[corner_blocks.index(corner)], goal).start()
        pl.when(condition)(start)
        sends.append((move(("corner", corner), block_ref(source_cell), XC.at[0], goal), condition))

    even = lax.rem(me_lat, 2) == 0
    odd = lax.rem(me_lat, 2) == 1
    lat_up = jnp.logical_and(odd, me_lat + 1 < count_lat)
    lat_down = jnp.logical_and(even, me_lat >= 1)

    def near_columns(side):
        for cell in near_cells(side):
            wait_block(cell)
        a, b = side
        if b == 0:
            x = 2 if a > 0 else -1
            relay(even, (x, 1), (a, -1), (0, 1))
            relay(odd, (x, 0), (a, 1), (0, -1))
        elif b == 1:
            relay(lat_up, (1, 2), (-1, 1), (1, 0))
            relay(lat_up, (0, 2), (1, 1), (-1, 0))
        else:
            relay(lat_down, (1, -1), (-1, -1), (1, 0))
            relay(lat_down, (0, -1), (1, -1), (-1, 0))
        for cell in near_cells(side):
            row = 4 if b == 0 else 5
            PT[cell_index[cell]] = (block_value(cell) * coef(cell, row)).T

    filled = set()

    def add(block, values):
        place = slot_of[block]
        if place in filled:
            out[place] = out[place] + values
        else:
            out[place] = values
            filled.add(place)

    def galerkin(cell):
        x, y = cell
        a, b = x // 2, y // 2
        applied = None
        if cell in support:
            own = PT[cell_index[cell]]
            applied = own * coef(cell, 6) + roll_down(own) * coef(cell, 7) + roll_up(own) * coef(cell, 8)
        for other in neighbours(cell):
            if other in support:
                term = PT[cell_index[other]] * edge(cell, other)
                applied = -term if applied is None else applied - term
        high, low = split(applied)
        left = jnp.concatenate([high, low], axis=1)
        high, low = split(block_value(cell))
        right = jnp.concatenate([high, low], axis=1)
        right = jnp.concatenate([right, right], axis=0)
        product = jnp.dot(left, right, preferred_element_type=jnp.float32)
        product = product[:, :128] + product[:, 128:]
        own = applied * coef(cell, 0) + product * coef(cell, 1)
        own = own + roll_down(product) * coef(cell, 2) + roll_up(product) * coef(cell, 3)
        add((a, b), own)
        add((a + (1 if x % 2 else -1), b), product * coef(cell, 4))
        add((a, b + (1 if y % 2 else -1)), product * coef(cell, 5))

    for side in sides:
        near_columns(side)
    for cell in support:
        galerkin(cell)
    for step in (0, 1):
        for side in sides:
            cell = far_cells(side)[step]
            wait_block(cell)
            galerkin(cell)
    for block in corner_blocks:
        p, r = corner_cell(block)
        cell = (2 * block[0] + p, 2 * block[1] + r)
        landing = XC.at[corner_blocks.index(block)]
        copy = move(("corner", block), X.at[0, 0, 0], landing, (block[0], 0))
        pl.when(exists(block))(copy.wait_recv)
        galerkin(cell)
    assert len(filled) == len(offsets)
    for copy, condition in sends:
        only(condition, copy.wait_send)


def local(inverse, vert_diag, vert_coup, face_east, face_north, land_mask, aggregate):
    blocks = len(offsets)
    messages = len(message)
    coarse = pl.pallas_call(
        kernel,
        out_shape=jax.ShapeDtypeStruct((blocks, 128, 128), jnp.float32),
        in_specs=[pl.BlockSpec(memory_space=pl.ANY)] * 7,
        out_specs=pl.BlockSpec(memory_space=pltpu.VMEM),
        scratch_shapes=[
            pltpu.VMEM((5, 2, 2, 128, 128), jnp.float32),
            pltpu.VMEM((4, 128, 128), jnp.float32),
            pltpu.VMEM((5, 24, 128), jnp.float32),
            pltpu.VMEM((4, 8, 128), jnp.float32),
            pltpu.VMEM((4, 8, 128), jnp.float32),
            pltpu.VMEM((4, 8, 128), jnp.float32),
            pltpu.VMEM((4, 2, 2, 128), jnp.float32),
            pltpu.VMEM((2, 2, 2), jnp.int32),
            pltpu.VMEM((len(support), 128, 128), jnp.float32),
            pltpu.VMEM((coef_rows, 128), jnp.float32),
            pltpu.SemaphoreType.DMA((7,)),
            pltpu.SemaphoreType.DMA((messages,)),
            pltpu.SemaphoreType.DMA((messages,)),
        ],
        compiler_params=pltpu.CompilerParams(collective_id=0, has_side_effects=True),
    )(inverse, vert_diag, vert_coup, face_east, face_north, land_mask, aggregate)
    return coarse[None, None]


def solution(mesh):
    return jax.shard_map(
        local,
        mesh=mesh,
        in_specs=(
            P("lon", "lat", None, None),
            P("lon", "lat", None),
            P("lon", "lat", None),
            P("lon", "lat", None),
            P("lon", "lat", None),
            P("lon", "lat"),
            P("lon", "lat"),
        ),
        out_specs=P("lon", "lat", None, None, None),
        check_vma=False,
    )
```

```python
import jax
import jax.numpy as jnp
from jax import lax
from jax.experimental import pallas as pl
from jax.experimental.pallas import tpu as pltpu
from jax.sharding import PartitionSpec as P

MESH = pl.DeviceIdType.MESH
relax = 0.6
offsets = [
    (-2, 0),
    (-1, -1),
    (-1, 0),
    (-1, 1),
    (0, -2),
    (0, -1),
    (0, 0),
    (0, 1),
    (0, 2),
    (1, -1),
    (1, 0),
    (1, 1),
    (2, 0),
]
slot_of = {offset: place for place, offset in enumerate(offsets)}
near_blocks = [(0, 0), (1, 0), (-1, 0), (0, 1), (0, -1)]
second_blocks = [(2, 0), (-2, 0), (0, 2), (0, -2)]
corner_blocks = [(1, 1), (-1, 1), (1, -1), (-1, -1)]
packet_blocks = near_blocks + corner_blocks
sides = [(1, 0), (-1, 0), (0, 1), (0, -1)]


def corner_cell(block):
    return (0 if block[0] > 0 else 1, 0 if block[1] > 0 else 1)


def cells_of(block):
    return [(2 * block[0] + p, 2 * block[1] + r) for p in (0, 1) for r in (0, 1)]


def near_cells(side):
    a, b = side
    if b == 0:
        p = 0 if a > 0 else 1
        return [(2 * a + p, r) for r in (0, 1)]
    r = 0 if b > 0 else 1
    return [(p, 2 * b + r) for p in (0, 1)]


def far_cells(side):
    near = near_cells(side)
    return [cell for cell in cells_of(side) if cell not in near]


def neighbours(cell):
    x, y = cell
    return [(x + 1, y), (x - 1, y), (x, y + 1), (x, y - 1)]


own_cells = cells_of((0, 0))
support = own_cells + [cell for side in sides for cell in near_cells(side)]
outer = [cell for side in sides for cell in far_cells(side)] + [
    (2 * a + corner_cell((a, b))[0], 2 * b + corner_cell((a, b))[1]) for a, b in corner_blocks
]
all_cells = support + outer
cell_index = {cell: place for place, cell in enumerate(all_cells)}
COEFS = 9
edge_list = []
for cell in support:
    for other in neighbours(cell):
        key = tuple(sorted((cell, other)))
        if key not in edge_list:
            edge_list.append(key)
edge_index = {edge: COEFS * len(all_cells) + place for place, edge in enumerate(edge_list)}
coef_rows = COEFS * len(all_cells) + len(edge_list)
coef_rows = (coef_rows + 7) // 8 * 8

message = {}
for block in near_blocks[1:] + second_blocks + corner_blocks:
    message["packet", block] = len(message)
for side in sides:
    for cell in near_cells(side) + far_cells(side):
        message["block", cell] = len(message)
for block in corner_blocks:
    message["corner", block] = len(message)


def down(values):
    lane = lax.broadcasted_iota(jnp.int32, values.shape, 1)
    return jnp.where(lane > 0, pltpu.roll(values, 1, 1), 0.0)


def split(values):
    high = values.astype(jnp.bfloat16)
    low = (values - high.astype(jnp.float32)).astype(jnp.bfloat16)
    return high, low


def kernel(
    inv_h, vd_h, vc_h, fe_h, fn_h, land_h, agg_h,
    out,
    X, XC, PK, PC, SM, LA, PT, CF,
    local_sem, send_sem, recv_sem,
):
    me_lon = lax.axis_index("lon")
    me_lat = lax.axis_index("lat")
    count_lon = lax.axis_size("lon")
    count_lat = lax.axis_size("lat")
    own_of = {"vd": 0, "vc": 1, "fe": 2, "fn": 3}
    east, west, north, south = sides

    small_copies = [
        pltpu.make_async_copy(source, SM.at[place], local_sem.at[1 + place])
        for place, source in enumerate((vd_h, vc_h, fe_h, fn_h))
    ] + [
        pltpu.make_async_copy(source, LA.at[place], local_sem.at[5 + place])
        for place, source in enumerate((land_h, agg_h))
    ]
    inverse_copy = pltpu.make_async_copy(inv_h, X.at[0], local_sem.at[0])
    for copy in small_copies:
        copy.start()
    inverse_copy.start()

    def target(block):
        a, b = block
        return {"lon": lax.rem(me_lon + a + count_lon, count_lon), "lat": me_lat + b}

    def exists(block):
        b = block[1]
        if b == 0:
            return None
        return me_lat + b < count_lat if b > 0 else me_lat + b >= 0

    def both(first, second):
        if first is None:
            return second
        return first if second is None else jnp.logical_and(first, second)

    def only(condition, action):
        if condition is None:
            action()
        else:
            pl.when(condition)(action)

    barrier = pltpu.get_barrier_semaphore()
    for block in (west, north, south):
        def signal(block=block):
            pl.semaphore_signal(barrier, inc=1, device_id=target(block), device_id_type=MESH)
        only(exists(block), signal)

    partners = near_blocks[1:] + second_blocks + corner_blocks
    for block in partners:
        if block[1] == 0:
            continue
        def clear(block=block):
            if block in second_blocks:
                PC[second_blocks.index(block)] = jnp.zeros((8, 128), jnp.float32)
                return
            PK[packet_blocks.index(block)] = jnp.zeros((24, 128), jnp.float32)
            if block in near_blocks:
                X[near_blocks.index(block)] = jnp.zeros((2, 2, 128, 128), jnp.float32)
            else:
                XC[corner_blocks.index(block)] = jnp.zeros((128, 128), jnp.float32)
        pl.when(jnp.logical_not(exists(block)))(clear)

    for copy in small_copies:
        copy.wait()
    live = (LA[1] >= 0).astype(jnp.float32)
    land = LA[0].astype(jnp.float32)

    def spread(values, p, r):
        return jnp.broadcast_to(values[p : p + 1, r : r + 1], (1, 128))

    lives = {(p, r): spread(live, p, r) for p in (0, 1) for r in (0, 1)}
    block_count = lives[0, 0] + lives[0, 1] + lives[1, 0] + lives[1, 1]
    norm = jnp.sqrt(jnp.maximum(block_count, 1.0))
    lane = lax.broadcasted_iota(jnp.int32, (1, 128), 1)
    scalars = jnp.zeros((1, 128), jnp.float32)
    for p in (0, 1):
        for r in (0, 1):
            scalars = jnp.where(lane == 2 * p + r, spread(land, p, r), scalars)
            scalars = jnp.where(lane == 4 + 2 * p + r, lives[p, r] / norm, scalars)

    def mine(field, p, r):
        return SM[own_of[field], p, pl.ds(r, 1), :]

    blank = jnp.zeros((1, 128), jnp.float32)
    head = [scalars, mine("fe", 1, 0), mine("fe", 1, 1), mine("fn", 0, 1), mine("fn", 1, 1)]
    for row, values in enumerate(head + [blank] * 3):
        PK[0, pl.ds(row, 1), :] = values
    for first, field in ((8, "fe"), (12, "fn"), (16, "vd"), (20, "vc")):
        for p in (0, 1):
            for r in (0, 1):
                PK[0, pl.ds(first + 2 * p + r, 1), :] = mine(field, p, r)

    lat_count = jnp.where(me_lat + 1 < count_lat, 1, 0) + jnp.where(me_lat >= 1, 1, 0)
    pl.semaphore_wait(barrier, 1 + lat_count)

    sends = []

    def move(key, source, landing, block):
        place = message[key]
        return pltpu.make_async_remote_copy(
            src_ref=source,
            dst_ref=landing,
            send_sem=send_sem.at[place],
            recv_sem=recv_sem.at[place],
            device_id=target(block),
            device_id_type=MESH,
        )

    def opposite(block):
        return (-block[0], -block[1])

    def packet_ref(block):
        if block in second_blocks:
            return PC.at[second_blocks.index(block)]
        return PK.at[packet_blocks.index(block)]

    def block_ref(cell):
        x, y = cell
        block = (x // 2, y // 2)
        if block in near_blocks:
            return X.at[near_blocks.index(block), x % 2, y % 2]
        return XC.at[corner_blocks.index(block)]

    def block_value(cell):
        x, y = cell
        block = (x // 2, y // 2)
        if block in near_blocks:
            return X[near_blocks.index(block), x % 2, y % 2]
        return XC[corner_blocks.index(block)]

    def corner_of(block):
        p, r = corner_cell(block)
        return (2 * block[0] + p, 2 * block[1] + r)

    def send(key, source, landing, goal, condition):
        copy = move(key, source, landing, goal)
        only(condition, copy.start)
        sends.append((copy, condition))
        return copy

    def send_packet(goal):
        seen = opposite(goal)
        send(("packet", seen), PK.at[0], packet_ref(seen), goal, exists(goal))

    def send_blocks(goal, cells):
        seen = opposite(goal)
        for cell in cells(seen):
            source = X.at[0, cell[0] % 2, cell[1] % 2]
            send(("block", cell), source, block_ref(cell), goal, exists(goal))

    def relay_packet(block):
        for goal in sides:
            if goal == block or (block[0] == 0 and goal[1] == 0):
                continue
            seen = (block[0] - goal[0], block[1] - goal[1])
            condition = both(exists(block), exists(goal))
            source = packet_ref(block)
            if seen in second_blocks:
                source = PK.at[packet_blocks.index(block), pl.ds(0, 8)]
            send(("packet", seen), source, packet_ref(seen), goal, condition)

    def relay_corners(block):
        for goal in (north, south):
            seen = (block[0], -goal[1])
            cell = corner_of(seen)
            source = block_ref((cell[0], cell[1] + 2 * goal[1]))
            send(("corner", seen), source, block_ref(cell), goal, exists(goal))

    def wait(key, source, landing, origin, condition):
        only(condition, move(key, source, landing, origin).wait_recv)

    def wait_packet(block, origin=None):
        landing = packet_ref(block)
        source = PK.at[0, pl.ds(0, 8)] if block in second_blocks else PK.at[0]
        wait(("packet", block), source, landing, origin or block, exists(block))

    def wait_block(cell):
        block = (cell[0] // 2, cell[1] // 2)
        wait(("block", cell), X.at[0, 0, 0], block_ref(cell), block, exists(block))

    for goal in (east, north, south):
        send_packet(goal)
    inverse_copy.wait()
    for cells in (near_cells, far_cells):
        send_blocks(east, cells)
    for cells in (near_cells, far_cells):
        for goal in (north, south):
            send_blocks(goal, cells)
    wait_packet(west)
    send_packet(west)
    for cells in (near_cells, far_cells):
        send_blocks(west, cells)
    for block in (west, east, north, south):
        if block != west:
            wait_packet(block)
        relay_packet(block)

    cache = {}

    def field(name, cell):
        if (name, cell) in cache:
            return cache[name, cell]
        x, y = cell
        block = (x // 2, y // 2)
        p, r = x % 2, y % 2
        place = 2 * p + r
        if block in second_blocks:
            ref, at = PC, second_blocks.index(block)
            row = {"fe": 1 + r, "fn": 3 + p}.get(name, 0)
            assert (name != "fe" or p == 1) and (name != "fn" or r == 1)
        else:
            ref, at = PK, packet_blocks.index(block)
            row = {"fe": 8, "fn": 12, "vd": 16, "vc": 20}.get(name, 0) + place
        if name in ("land", "w"):
            lane_at = place + (4 if name == "w" else 0)
            row_values = ref[at, pl.ds(0, 1), :]
            value = jnp.broadcast_to(row_values[:, lane_at : lane_at + 1], (1, 128))
        else:
            value = ref[at, pl.ds(row, 1), :]
        cache[name, cell] = value
        return value

    def face(low, high):
        if ("face", low, high) not in cache:
            name = "fe" if low[1] == high[1] else "fn"
            cache["face", low, high] = field(name, low) * (field("land", low) * field("land", high))
        return cache["face", low, high]

    def between(cell, other):
        return face(*sorted((cell, other)))

    def coef(cell, row):
        return CF[pl.ds(COEFS * cell_index[cell] + row, 1), :]

    def edge(cell, other):
        return CF[pl.ds(edge_index[tuple(sorted((cell, other)))], 1), :]

    top = lax.broadcasted_iota(jnp.int32, (1, 128), 1) < 127

    def make_coefs(cell):
        x, y = cell
        p, r = x % 2, y % 2
        lon_cross, lon_same = ((x - 1, y), (x + 1, y)) if p == 0 else ((x + 1, y), (x - 1, y))
        lat_cross, lat_same = ((x, y - 1), (x, y + 1)) if r == 0 else ((x, y + 1), (x, y - 1))
        w = field("w", cell)
        vc = field("vc", cell)
        main = field("vd", cell) + vc + down(vc)
        for other in neighbours(cell):
            main = main + between(cell, other)
        same = between(cell, lon_same) * field("w", lon_same)
        same = same + between(cell, lat_same) * field("w", lat_same)
        weighted = w * main - same
        up = jnp.where(top, vc, 0.0)
        below = down(up)
        rows = [
            w,
            -relax * weighted,
            relax * w * below,
            relax * w * up,
            relax * between(cell, lon_cross) * field("w", lon_cross),
            relax * between(cell, lat_cross) * field("w", lat_cross),
        ]
        if cell in support:
            rows += [main, -below, -up]
        for row, values in enumerate(rows):
            CF[pl.ds(COEFS * cell_index[cell] + row, 1), :] = values

    for cell in own_cells:
        make_coefs(cell)

    def roll_down(values):
        return pltpu.roll(values, 1, 1)

    def roll_up(values):
        return pltpu.roll(values, 127, 1)

    diagonal = lax.broadcasted_iota(jnp.int32, (128, 128), 0) == lax.broadcasted_iota(
        jnp.int32, (128, 128), 1
    )
    for cell in own_cells:
        inverse = block_value(cell)
        values = jnp.where(diagonal, coef(cell, 0), 0.0) + inverse * coef(cell, 1)
        values = values + roll_down(inverse) * coef(cell, 2) + roll_up(inverse) * coef(cell, 3)
        PT[cell_index[cell]] = values.T

    for block in second_blocks[:1] + second_blocks[2:]:
        wait_packet(block, (block[0] // 2, block[1] // 2))
    for block in corner_blocks:
        wait_packet(block, (0, block[1]))
    late_cells = far_cells(west)
    for cell in all_cells:
        if cell not in own_cells and cell not in late_cells:
            make_coefs(cell)
    for low, high in edge_list:
        CF[pl.ds(edge_index[low, high], 1), :] = face(low, high)

    def near_columns(side):
        for cell in near_cells(side):
            wait_block(cell)
        if side in (east, west):
            relay_corners(side)
        for cell in near_cells(side):
            row = 4 if side in (east, west) else 5
            PT[cell_index[cell]] = (block_value(cell) * coef(cell, row)).T

    filled = set()

    def add(block, values):
        place = slot_of[block]
        if place in filled:
            out[place] = out[place] + values
        else:
            out[place] = values
            filled.add(place)

    def galerkin(cell):
        x, y = cell
        a, b = x // 2, y // 2
        applied = None
        if cell in support:
            own = PT[cell_index[cell]]
            applied = own * coef(cell, 6) + roll_down(own) * coef(cell, 7) + roll_up(own) * coef(cell, 8)
        for other in neighbours(cell):
            if other in support:
                term = PT[cell_index[other]] * edge(cell, other)
                applied = -term if applied is None else applied - term
        high, low = split(applied)
        left = jnp.concatenate([high, low], axis=1)
        high, low = split(block_value(cell))
        right = jnp.concatenate([high, low], axis=1)
        right = jnp.concatenate([right, right], axis=0)
        product = jnp.dot(left, right, preferred_element_type=jnp.float32)
        product = product[:, :128] + product[:, 128:]
        own = applied * coef(cell, 0) + product * coef(cell, 1)
        own = own + roll_down(product) * coef(cell, 2) + roll_up(product) * coef(cell, 3)
        add((a, b), own)
        add((a + (1 if x % 2 else -1), b), product * coef(cell, 4))
        add((a, b + (1 if y % 2 else -1)), product * coef(cell, 5))

    def corner(block):
        landing = XC.at[corner_blocks.index(block)]
        wait(("corner", block), X.at[0, 0, 0], landing, (0, block[1]), exists(block))
        galerkin(corner_of(block))

    for side in (east, north, south):
        near_columns(side)
    for side in (east, north, south):
        for cell in near_cells(side):
            galerkin(cell)
    for cell in own_cells[2:]:
        galerkin(cell)
    for side in (east, north, south):
        for cell in far_cells(side):
            wait_block(cell)
            galerkin(cell)
    for block in corner_blocks:
        if block[0] > 0:
            corner(block)
    near_columns(west)
    for cell in own_cells[:2] + near_cells(west):
        galerkin(cell)
    wait_packet((-2, 0), west)
    for cell in late_cells:
        make_coefs(cell)
    for cell in late_cells:
        wait_block(cell)
        galerkin(cell)
    for block in corner_blocks:
        if block[0] < 0:
            corner(block)
    assert len(filled) == len(offsets)
    for copy, condition in sends:
        only(condition, copy.wait_send)


def publish(held, out, sem):
    copies = [
        pltpu.make_async_copy(held.at[place], out.at[place], sem.at[place])
        for place in range(len(offsets))
    ]
    for copy in copies:
        copy.start()
    for copy in copies:
        copy.wait()


def local(inverse, vert_diag, vert_coup, face_east, face_north, land_mask, aggregate):
    blocks = len(offsets)
    messages = len(message)
    anywhere = pl.BlockSpec(memory_space=pltpu.HBM)
    held = pl.pallas_call(
        kernel,
        out_shape=pltpu.VMEM((blocks, 128, 128), jnp.float32),
        in_specs=[anywhere] * 7,
        out_specs=pl.BlockSpec(memory_space=pltpu.VMEM),
        scratch_shapes=[
            pltpu.VMEM((5, 2, 2, 128, 128), jnp.float32),
            pltpu.VMEM((4, 128, 128), jnp.float32),
            pltpu.VMEM((9, 24, 128), jnp.float32),
            pltpu.VMEM((4, 8, 128), jnp.float32),
            pltpu.VMEM((4, 2, 2, 128), jnp.float32),
            pltpu.VMEM((2, 2, 2), jnp.int32),
            pltpu.VMEM((len(support), 128, 128), jnp.float32),
            pltpu.VMEM((coef_rows, 128), jnp.float32),
            pltpu.SemaphoreType.DMA((7,)),
            pltpu.SemaphoreType.DMA((messages,)),
            pltpu.SemaphoreType.DMA((messages,)),
        ],
        compiler_params=pltpu.CompilerParams(collective_id=0, has_side_effects=True),
    )(inverse, vert_diag, vert_coup, face_east, face_north, land_mask, aggregate)
    coarse = pl.pallas_call(
        publish,
        out_shape=jax.ShapeDtypeStruct((blocks, 128, 128), jnp.float32),
        in_specs=[pl.BlockSpec(memory_space=pltpu.VMEM)],
        out_specs=anywhere,
        scratch_shapes=[pltpu.SemaphoreType.DMA((blocks,))],
        compiler_params=pltpu.CompilerParams(vmem_limit_bytes=2**20),
    )(held)
    return coarse[None, None]


def solution(mesh):
    return jax.shard_map(
        local,
        mesh=mesh,
        in_specs=(
            P("lon", "lat", None, None),
            P("lon", "lat", None),
            P("lon", "lat", None),
            P("lon", "lat", None),
            P("lon", "lat", None),
            P("lon", "lat"),
            P("lon", "lat"),
        ),
        out_specs=P("lon", "lat", None, None, None),
        check_vma=False,
    )
```

```python
import jax
import jax.numpy as jnp
from jax import lax
from jax.experimental import pallas as pl
from jax.experimental.pallas import tpu as pltpu
from jax.sharding import PartitionSpec as P

MESH = pl.DeviceIdType.MESH
relax = 0.6
offsets = [
    (-2, 0),
    (-1, -1),
    (-1, 0),
    (-1, 1),
    (0, -2),
    (0, -1),
    (0, 0),
    (0, 1),
    (0, 2),
    (1, -1),
    (1, 0),
    (1, 1),
    (2, 0),
]
slot_of = {offset: place for place, offset in enumerate(offsets)}
near_blocks = [(0, 0), (1, 0), (-1, 0), (0, 1), (0, -1)]
second_blocks = [(2, 0), (-2, 0), (0, 2), (0, -2)]
corner_blocks = [(1, 1), (-1, 1), (1, -1), (-1, -1)]
packet_blocks = near_blocks + corner_blocks
sides = [(1, 0), (-1, 0), (0, 1), (0, -1)]


def corner_cell(block):
    return (0 if block[0] > 0 else 1, 0 if block[1] > 0 else 1)


def cells_of(block):
    return [(2 * block[0] + p, 2 * block[1] + r) for p in (0, 1) for r in (0, 1)]


def near_cells(side):
    a, b = side
    if b == 0:
        p = 0 if a > 0 else 1
        return [(2 * a + p, r) for r in (0, 1)]
    r = 0 if b > 0 else 1
    return [(p, 2 * b + r) for p in (0, 1)]


def far_cells(side):
    near = near_cells(side)
    return [cell for cell in cells_of(side) if cell not in near]


def neighbours(cell):
    x, y = cell
    return [(x + 1, y), (x - 1, y), (x, y + 1), (x, y - 1)]


own_cells = cells_of((0, 0))
support = own_cells + [cell for side in sides for cell in near_cells(side)]
outer = [cell for side in sides for cell in far_cells(side)] + [
    (2 * a + corner_cell((a, b))[0], 2 * b + corner_cell((a, b))[1]) for a, b in corner_blocks
]
all_cells = support + outer
cell_index = {cell: place for place, cell in enumerate(all_cells)}
COEFS = 9
edge_list = []
for cell in support:
    for other in neighbours(cell):
        key = tuple(sorted((cell, other)))
        if key not in edge_list:
            edge_list.append(key)
edge_index = {edge: COEFS * len(all_cells) + place for place, edge in enumerate(edge_list)}
coef_rows = COEFS * len(all_cells) + len(edge_list)
coef_rows = (coef_rows + 7) // 8 * 8

message = {}
for block in near_blocks[1:] + second_blocks + corner_blocks:
    message["packet", block] = len(message)
for side in sides:
    for cell in near_cells(side) + far_cells(side):
        message["block", cell] = len(message)
for block in corner_blocks:
    message["corner", block] = len(message)


def down(values):
    lane = lax.broadcasted_iota(jnp.int32, values.shape, 1)
    return jnp.where(lane > 0, pltpu.roll(values, 1, 1), 0.0)


def split(values):
    high = values.astype(jnp.bfloat16)
    low = (values - high.astype(jnp.float32)).astype(jnp.bfloat16)
    return high, low


def kernel(
    inv_h, vd_h, vc_h, fe_h, fn_h, land_h, agg_h,
    out,
    X, XC, PK, PC, SM, LA, PT, CF,
    local_sem, send_sem, recv_sem,
):
    me_lon = lax.axis_index("lon")
    me_lat = lax.axis_index("lat")
    count_lon = lax.axis_size("lon")
    count_lat = lax.axis_size("lat")
    own_of = {"vd": 0, "vc": 1, "fe": 2, "fn": 3}
    east, west, north, south = sides

    small_copies = [
        pltpu.make_async_copy(source, SM.at[place], local_sem.at[1 + place])
        for place, source in enumerate((vd_h, vc_h, fe_h, fn_h))
    ] + [
        pltpu.make_async_copy(source, LA.at[place], local_sem.at[5 + place])
        for place, source in enumerate((land_h, agg_h))
    ]
    inverse_copy = pltpu.make_async_copy(inv_h, X.at[0], local_sem.at[0])
    for copy in small_copies:
        copy.start()
    inverse_copy.start()

    def target(block):
        a, b = block
        return {"lon": lax.rem(me_lon + a + count_lon, count_lon), "lat": me_lat + b}

    inside = {b: me_lat + b < count_lat if b > 0 else me_lat + b >= 0 for b in (-2, -1, 1, 2)}

    def exists(block):
        return inside.get(block[1])

    def both(first, second):
        if first is None:
            return second
        return first if second is None else jnp.logical_and(first, second)

    def only(condition, action):
        if condition is None:
            action()
        else:
            pl.when(condition)(action)

    phase = lax.rem(me_lon, 64)
    late = phase == 0
    early = jnp.logical_not(late)
    even = lax.rem(me_lat, 2) == 0
    odd = lax.rem(me_lat, 2) == 1
    across_up = jnp.logical_and(odd, me_lat + 1 < count_lat)
    across_down = jnp.logical_and(even, me_lat >= 1)
    barrier = pltpu.get_barrier_semaphore()
    for block in near_blocks[1:] + second_blocks + corner_blocks:
        reach = None
        if block[0] > 0:
            reach = phase < 64 - block[0]
        def signal(block=block):
            pl.semaphore_signal(barrier, inc=1, device_id=target(block), device_id_type=MESH)
        only(both(exists(block), reach), signal)

    partners = near_blocks[1:] + second_blocks + corner_blocks
    for block in partners:
        if block[1] == 0:
            continue
        def clear(block=block):
            if block in second_blocks:
                PC[second_blocks.index(block)] = jnp.zeros((8, 128), jnp.float32)
                return
            PK[packet_blocks.index(block)] = jnp.zeros((24, 128), jnp.float32)
            if block in near_blocks:
                X[near_blocks.index(block)] = jnp.zeros((2, 2, 128, 128), jnp.float32)
            else:
                XC[corner_blocks.index(block)] = jnp.zeros((128, 128), jnp.float32)
        pl.when(jnp.logical_not(exists(block)))(clear)

    for copy in small_copies:
        copy.wait()
    live = (LA[1] >= 0).astype(jnp.float32)
    land = LA[0].astype(jnp.float32)

    def spread(values, p, r):
        return jnp.broadcast_to(values[p : p + 1, r : r + 1], (1, 128))

    lives = {(p, r): spread(live, p, r) for p in (0, 1) for r in (0, 1)}
    block_count = lives[0, 0] + lives[0, 1] + lives[1, 0] + lives[1, 1]
    norm = jnp.sqrt(jnp.maximum(block_count, 1.0))
    lane = lax.broadcasted_iota(jnp.int32, (1, 128), 1)
    scalars = jnp.zeros((1, 128), jnp.float32)
    for p in (0, 1):
        for r in (0, 1):
            scalars = jnp.where(lane == 2 * p + r, spread(land, p, r), scalars)
            scalars = jnp.where(lane == 4 + 2 * p + r, lives[p, r] / norm, scalars)

    def mine(field, p, r):
        return SM[own_of[field], p, pl.ds(r, 1), :]

    blank = jnp.zeros((1, 128), jnp.float32)
    head = [scalars, mine("fe", 1, 0), mine("fe", 1, 1), mine("fn", 0, 1), mine("fn", 1, 1)]
    for row, values in enumerate(head + [blank] * 3):
        PK[0, pl.ds(row, 1), :] = values
    for first, field in ((8, "fe"), (12, "fn"), (16, "vd"), (20, "vc")):
        for p in (0, 1):
            for r in (0, 1):
                PK[0, pl.ds(first + 2 * p + r, 1), :] = mine(field, p, r)

    lat_near = jnp.where(inside[1], 1, 0) + jnp.where(inside[-1], 1, 0)
    lat_second = jnp.where(inside[2], 1, 0) + jnp.where(inside[-2], 1, 0)
    awaited = 2 + 2 * lat_near + lat_second + jnp.where(early, 1 + lat_near, 0)
    pl.semaphore_wait(barrier, awaited + jnp.where(phase > 1, 1, 0))

    sends = []

    def move(key, source, landing, block):
        place = message[key]
        return pltpu.make_async_remote_copy(
            src_ref=source,
            dst_ref=landing,
            send_sem=send_sem.at[place],
            recv_sem=recv_sem.at[place],
            device_id=target(block),
            device_id_type=MESH,
        )

    def opposite(block):
        return (-block[0], -block[1])

    def packet_ref(block):
        if block in second_blocks:
            return PC.at[second_blocks.index(block)]
        return PK.at[packet_blocks.index(block)]

    def block_ref(cell):
        x, y = cell
        block = (x // 2, y // 2)
        if block in near_blocks:
            return X.at[near_blocks.index(block), x % 2, y % 2]
        return XC.at[corner_blocks.index(block)]

    def block_value(cell):
        x, y = cell
        block = (x // 2, y // 2)
        if block in near_blocks:
            return X[near_blocks.index(block), x % 2, y % 2]
        return XC[corner_blocks.index(block)]

    def corner_of(block):
        p, r = corner_cell(block)
        return (2 * block[0] + p, 2 * block[1] + r)

    listed = set()

    def send(key, source, landing, goal, condition):
        copy = move(key, source, landing, goal)
        only(condition, copy.start)
        if (key, goal) not in listed:
            sends.append((key, goal, exists(goal) if key[0] != "corner" else condition))
            listed.add((key, goal))

    def send_packet(goal, condition=None):
        seen = opposite(goal)
        source = PK.at[0, pl.ds(0, 8)] if seen in second_blocks else PK.at[0]
        send(("packet", seen), source, packet_ref(seen), goal, both(exists(goal), condition))

    def send_blocks(goal, cells, condition=None):
        seen = opposite(goal)
        for cell in cells(seen):
            source = X.at[0, cell[0] % 2, cell[1] % 2]
            send(("block", cell), source, block_ref(cell), goal, both(exists(goal), condition))

    def mate(goal):
        return even if goal == north else odd

    def relay_corners(block):
        for goal in (north, south):
            seen = (block[0], -goal[1])
            cell = corner_of(seen)
            source = block_ref((cell[0], cell[1] + 2 * goal[1]))
            condition = mate(goal) if block == west else exists(goal)
            send(("corner", seen), source, block_ref(cell), goal, condition)

    def send_across(goal, condition):
        seen = opposite(goal)
        cell = corner_of(seen)
        source = X.at[0, cell[0] % 2, cell[1] % 2]
        send(("corner", seen), source, block_ref(cell), goal, condition)

    def wait(key, source, landing, origin, condition):
        only(condition, move(key, source, landing, origin).wait_recv)

    def wait_packet(block):
        landing = packet_ref(block)
        source = PK.at[0, pl.ds(0, 8)] if block in second_blocks else PK.at[0]
        wait(("packet", block), source, landing, block, exists(block))

    def wait_block(cell):
        block = (cell[0] // 2, cell[1] // 2)
        wait(("block", cell), X.at[0, 0, 0], block_ref(cell), block, exists(block))

    def serve(goal, condition=None):
        for cells in (near_cells, far_cells):
            send_blocks(goal, cells, condition)

    west_side = [west, (-1, 1), (-1, -1)]
    for goal in (east, (2, 0), (1, 1), (1, -1), north, south, (0, 2), (0, -2)):
        send_packet(goal)
    for goal in west_side:
        send_packet(goal, early)
    send_packet((-2, 0), phase > 1)
    inverse_copy.wait()
    send_across((1, 1), across_up)
    send_across((1, -1), across_down)
    serve(east)
    for cells in (near_cells, far_cells):
        send_blocks(west, cells, early)
        send_blocks(north, cells)
        send_blocks(south, cells)

    cache = {}

    def field(name, cell):
        if (name, cell) in cache:
            return cache[name, cell]
        x, y = cell
        block = (x // 2, y // 2)
        p, r = x % 2, y % 2
        place = 2 * p + r
        if block in second_blocks:
            ref, at = PC, second_blocks.index(block)
            row = {"fe": 1 + r, "fn": 3 + p}.get(name, 0)
            assert (name != "fe" or p == 1) and (name != "fn" or r == 1)
        else:
            ref, at = PK, packet_blocks.index(block)
            row = {"fe": 8, "fn": 12, "vd": 16, "vc": 20}.get(name, 0) + place
        if name in ("land", "w"):
            lane_at = place + (4 if name == "w" else 0)
            row_values = ref[at, pl.ds(0, 1), :]
            value = jnp.broadcast_to(row_values[:, lane_at : lane_at + 1], (1, 128))
        else:
            value = ref[at, pl.ds(row, 1), :]
        cache[name, cell] = value
        return value

    def face(low, high):
        if ("face", low, high) not in cache:
            name = "fe" if low[1] == high[1] else "fn"
            cache["face", low, high] = field(name, low) * (field("land", low) * field("land", high))
        return cache["face", low, high]

    def between(cell, other):
        return face(*sorted((cell, other)))

    def coef(cell, row):
        return CF[pl.ds(COEFS * cell_index[cell] + row, 1), :]

    def edge(cell, other):
        return CF[pl.ds(edge_index[tuple(sorted((cell, other)))], 1), :]

    top = lax.broadcasted_iota(jnp.int32, (1, 128), 1) < 127

    def make_coefs(cell):
        x, y = cell
        p, r = x % 2, y % 2
        lon_cross, lon_same = ((x - 1, y), (x + 1, y)) if p == 0 else ((x + 1, y), (x - 1, y))
        lat_cross, lat_same = ((x, y - 1), (x, y + 1)) if r == 0 else ((x, y + 1), (x, y - 1))
        w = field("w", cell)
        vc = field("vc", cell)
        main = field("vd", cell) + vc + down(vc)
        for other in neighbours(cell):
            main = main + between(cell, other)
        same = between(cell, lon_same) * field("w", lon_same)
        same = same + between(cell, lat_same) * field("w", lat_same)
        weighted = w * main - same
        up = jnp.where(top, vc, 0.0)
        below = down(up)
        rows = [
            w,
            -relax * weighted,
            relax * w * below,
            relax * w * up,
            relax * between(cell, lon_cross) * field("w", lon_cross),
            relax * between(cell, lat_cross) * field("w", lat_cross),
        ]
        if cell in support:
            rows += [main, -below, -up]
        for row, values in enumerate(rows):
            CF[pl.ds(COEFS * cell_index[cell] + row, 1), :] = values

    def roll_down(values):
        return pltpu.roll(values, 1, 1)

    def roll_up(values):
        return pltpu.roll(values, 127, 1)

    diagonal = lax.broadcasted_iota(jnp.int32, (128, 128), 0) == lax.broadcasted_iota(
        jnp.int32, (128, 128), 1
    )

    def own_columns(cells):
        for cell in cells:
            inverse = block_value(cell)
            values = jnp.where(diagonal, coef(cell, 0), 0.0) + inverse * coef(cell, 1)
            values = values + roll_down(inverse) * coef(cell, 2) + roll_up(inverse) * coef(cell, 3)
            PT[cell_index[cell]] = values.T

    def near_columns(side):
        for cell in near_cells(side):
            inner = (cell[0] - side[0], cell[1] - side[1])
            scale = relax * between(cell, inner) * field("w", inner)
            PT[cell_index[cell]] = (block_value(cell) * scale).T

    def edges(early):
        for low, high in edge_list:
            if (high[0] >= 0 and low[0] >= 0) == early:
                CF[pl.ds(edge_index[low, high], 1), :] = face(low, high)

    filled = set()

    def add(block, values):
        place = slot_of[block]
        if place in filled:
            out[place] = out[place] + values
        else:
            out[place] = values
            filled.add(place)

    def galerkin(cell):
        x, y = cell
        a, b = x // 2, y // 2
        applied = None
        if cell in support:
            own = PT[cell_index[cell]]
            applied = own * coef(cell, 6) + roll_down(own) * coef(cell, 7) + roll_up(own) * coef(cell, 8)
        for other in neighbours(cell):
            if other in support:
                term = PT[cell_index[other]] * edge(cell, other)
                applied = -term if applied is None else applied - term
        high, low = split(applied)
        left = jnp.concatenate([high, low], axis=1)
        high, low = split(block_value(cell))
        right = jnp.concatenate([high, low], axis=1)
        right = jnp.concatenate([right, right], axis=0)
        product = jnp.dot(left, right, preferred_element_type=jnp.float32)
        product = product[:, :128] + product[:, 128:]
        own = applied * coef(cell, 0) + product * coef(cell, 1)
        own = own + roll_down(product) * coef(cell, 2) + roll_up(product) * coef(cell, 3)
        add((a, b), own)
        add((a + (1 if x % 2 else -1), b), product * coef(cell, 4))
        add((a, b + (1 if y % 2 else -1)), product * coef(cell, 5))

    def corner(block):
        landing = XC.at[corner_blocks.index(block)]
        wait(("corner", block), X.at[0, 0, 0], landing, (0, block[1]), exists(block))
        galerkin(corner_of(block))

    for block in (east, (2, 0), (1, 1), (1, -1), north, south, (0, 2), (0, -2)):
        wait_packet(block)
    for cell in all_cells:
        if cell[0] > 0:
            make_coefs(cell)
    edges(True)
    own_columns(own_cells[2:])
    for side in (north, south, east):
        for cell in near_cells(side):
            wait_block(cell)
        if side == east:
            relay_corners(side)
        near_columns(side)
    for cell in near_cells(east):
        galerkin(cell)
    for side in (north, south):
        galerkin(near_cells(side)[1])
        for cell in far_cells(side):
            wait_block(cell)
        galerkin(far_cells(side)[1])
    for cell in far_cells(east):
        wait_block(cell)
        galerkin(cell)
    for block in corner_blocks:
        if block[0] > 0:
            corner(block)

    for block in west_side + [(-2, 0)]:
        wait_packet(block)
        send_packet(block, phase <= 1 if block == (-2, 0) else late)
    for cell in all_cells:
        if cell[0] <= 0:
            make_coefs(cell)
    edges(False)
    own_columns(own_cells[:2])
    for cell in own_cells[2:]:
        galerkin(cell)
    for side in (north, south):
        for cell in (near_cells(side)[0], far_cells(side)[0]):
            galerkin(cell)
    for cell in near_cells(west):
        wait_block(cell)
    relay_corners(west)
    serve(west, late)
    near_columns(west)
    for cell in own_cells[:2] + near_cells(west):
        galerkin(cell)
    for cell in far_cells(west):
        wait_block(cell)
        galerkin(cell)
    for block in corner_blocks:
        if block[0] < 0:
            corner(block)
    assert len(filled) == len(offsets)
    for key, goal, condition in sends:
        def drain(key=key, goal=goal):
            source = X.at[0, 0, 0]
            if key[0] == "packet":
                source = PK.at[0, pl.ds(0, 8)] if key[1] in second_blocks else PK.at[0]
            move(key, source, source, goal).wait_send()
        only(condition, drain)


def publish(held, out, sem):
    copies = [
        pltpu.make_async_copy(held.at[place], out.at[place], sem.at[place])
        for place in range(len(offsets))
    ]
    for copy in copies:
        copy.start()
    for copy in copies:
        copy.wait()


def local(inverse, vert_diag, vert_coup, face_east, face_north, land_mask, aggregate):
    blocks = len(offsets)
    messages = len(message)
    anywhere = pl.BlockSpec(memory_space=pltpu.HBM)
    held = pl.pallas_call(
        kernel,
        out_shape=pltpu.VMEM((blocks, 128, 128), jnp.float32),
        in_specs=[anywhere] * 7,
        out_specs=pl.BlockSpec(memory_space=pltpu.VMEM),
        scratch_shapes=[
            pltpu.VMEM((5, 2, 2, 128, 128), jnp.float32),
            pltpu.VMEM((4, 128, 128), jnp.float32),
            pltpu.VMEM((9, 24, 128), jnp.float32),
            pltpu.VMEM((4, 8, 128), jnp.float32),
            pltpu.VMEM((4, 2, 2, 128), jnp.float32),
            pltpu.VMEM((2, 2, 2), jnp.int32),
            pltpu.VMEM((len(support), 128, 128), jnp.float32),
            pltpu.VMEM((coef_rows, 128), jnp.float32),
            pltpu.SemaphoreType.DMA((7,)),
            pltpu.SemaphoreType.DMA((messages,)),
            pltpu.SemaphoreType.DMA((messages,)),
        ],
        compiler_params=pltpu.CompilerParams(collective_id=0, has_side_effects=True),
    )(inverse, vert_diag, vert_coup, face_east, face_north, land_mask, aggregate)
    coarse = pl.pallas_call(
        publish,
        out_shape=jax.ShapeDtypeStruct((blocks, 128, 128), jnp.float32),
        in_specs=[pl.BlockSpec(memory_space=pltpu.VMEM)],
        out_specs=anywhere,
        scratch_shapes=[pltpu.SemaphoreType.DMA((blocks,))],
        compiler_params=pltpu.CompilerParams(vmem_limit_bytes=2**20),
    )(held)
    return coarse[None, None]


def solution(mesh):
    return jax.shard_map(
        local,
        mesh=mesh,
        in_specs=(
            P("lon", "lat", None, None),
            P("lon", "lat", None),
            P("lon", "lat", None),
            P("lon", "lat", None),
            P("lon", "lat", None),
            P("lon", "lat"),
            P("lon", "lat"),
        ),
        out_specs=P("lon", "lat", None, None, None),
        check_vma=False,
    )
```

```python
import jax
import jax.numpy as jnp
from jax import lax
from jax.experimental import pallas as pl
from jax.experimental.pallas import tpu as pltpu
from jax.sharding import PartitionSpec as P

MESH = pl.DeviceIdType.MESH
relax = 0.6
offsets = [
    (-2, 0),
    (-1, -1),
    (-1, 0),
    (-1, 1),
    (0, -2),
    (0, -1),
    (0, 0),
    (0, 1),
    (0, 2),
    (1, -1),
    (1, 0),
    (1, 1),
    (2, 0),
]
slot_of = {offset: place for place, offset in enumerate(offsets)}
near_blocks = [(0, 0), (1, 0), (-1, 0), (0, 1), (0, -1)]
second_blocks = [(2, 0), (-2, 0), (0, 2), (0, -2)]
corner_blocks = [(1, 1), (-1, 1), (1, -1), (-1, -1)]
packet_blocks = near_blocks + corner_blocks
sides = [(1, 0), (-1, 0), (0, 1), (0, -1)]


def corner_cell(block):
    return (0 if block[0] > 0 else 1, 0 if block[1] > 0 else 1)


def cells_of(block):
    return [(2 * block[0] + p, 2 * block[1] + r) for p in (0, 1) for r in (0, 1)]


def near_cells(side):
    a, b = side
    if b == 0:
        p = 0 if a > 0 else 1
        return [(2 * a + p, r) for r in (0, 1)]
    r = 0 if b > 0 else 1
    return [(p, 2 * b + r) for p in (0, 1)]


def far_cells(side):
    near = near_cells(side)
    return [cell for cell in cells_of(side) if cell not in near]


def neighbours(cell):
    x, y = cell
    return [(x + 1, y), (x - 1, y), (x, y + 1), (x, y - 1)]


own_cells = cells_of((0, 0))
support = own_cells + [cell for side in sides for cell in near_cells(side)]
outer = [cell for side in sides for cell in far_cells(side)] + [
    (2 * a + corner_cell((a, b))[0], 2 * b + corner_cell((a, b))[1]) for a, b in corner_blocks
]
all_cells = support + outer
cell_index = {cell: place for place, cell in enumerate(all_cells)}
COEFS = 9
edge_list = []
for cell in support:
    for other in neighbours(cell):
        key = tuple(sorted((cell, other)))
        if key not in edge_list:
            edge_list.append(key)
edge_index = {edge: COEFS * len(all_cells) + place for place, edge in enumerate(edge_list)}
coef_rows = COEFS * len(all_cells) + len(edge_list)
coef_rows = (coef_rows + 7) // 8 * 8

message = {}
for block in near_blocks[1:] + second_blocks + corner_blocks:
    message["packet", block] = len(message)
for side in sides:
    for cell in near_cells(side) + far_cells(side):
        message["block", cell] = len(message)
for block in corner_blocks:
    message["corner", block] = len(message)


def down(values):
    lane = lax.broadcasted_iota(jnp.int32, values.shape, 1)
    return jnp.where(lane > 0, pltpu.roll(values, 1, 1), 0.0)


def split(values):
    high = values.astype(jnp.bfloat16)
    low = (values - high.astype(jnp.float32)).astype(jnp.bfloat16)
    return high, low


def kernel(
    inv_h, vd_h, vc_h, fe_h, fn_h, land_h, agg_h,
    out,
    X, XC, PK, PC, SM, LA, PT, CF,
    local_sem, send_sem, recv_sem,
):
    me_lon = lax.axis_index("lon")
    me_lat = lax.axis_index("lat")
    count_lon = lax.axis_size("lon")
    count_lat = lax.axis_size("lat")
    own_of = {"vd": 0, "vc": 1, "fe": 2, "fn": 3}
    east, west, north, south = sides

    small_copies = [
        pltpu.make_async_copy(source, SM.at[place], local_sem.at[1 + place])
        for place, source in enumerate((vd_h, vc_h, fe_h, fn_h))
    ] + [
        pltpu.make_async_copy(source, LA.at[place], local_sem.at[5 + place])
        for place, source in enumerate((land_h, agg_h))
    ]
    inverse_copy = pltpu.make_async_copy(inv_h, X.at[0], local_sem.at[0])
    for copy in small_copies:
        copy.start()
    inverse_copy.start()

    def target(block):
        a, b = block
        return {"lon": lax.rem(me_lon + a + count_lon, count_lon), "lat": me_lat + b}

    inside = {b: me_lat + b < count_lat if b > 0 else me_lat + b >= 0 for b in (-2, -1, 1, 2)}

    def exists(block):
        return inside.get(block[1])

    def both(first, second):
        if first is None:
            return second
        return first if second is None else jnp.logical_and(first, second)

    def only(condition, action):
        if condition is None:
            action()
        else:
            pl.when(condition)(action)

    phase = lax.rem(me_lon, 64)
    late = phase == 0
    rim = phase == 63
    inner = phase < 63
    even = lax.rem(me_lat, 2) == 0
    odd = lax.rem(me_lat, 2) == 1
    across_up = jnp.logical_and(odd, me_lat + 1 < count_lat)
    across_down = jnp.logical_and(even, me_lat >= 1)
    barrier = pltpu.get_barrier_semaphore()
    for block in near_blocks[1:] + second_blocks + corner_blocks:
        reach = None
        if block[0] > 0:
            reach = phase < 63 - block[0]
        elif block == (0, 1):
            reach = jnp.logical_or(inner, odd)
        elif block == (0, -1):
            reach = jnp.logical_or(inner, odd)
        elif block == (0, -2):
            reach = inner
        def signal(block=block):
            pl.semaphore_signal(barrier, inc=1, device_id=target(block), device_id_type=MESH)
        only(both(exists(block), reach), signal)

    partners = near_blocks[1:] + second_blocks + corner_blocks
    for block in partners:
        if block[1] == 0:
            continue
        def clear(block=block):
            if block in second_blocks:
                PC[second_blocks.index(block)] = jnp.zeros((8, 128), jnp.float32)
                return
            PK[packet_blocks.index(block)] = jnp.zeros((24, 128), jnp.float32)
            if block in near_blocks:
                X[near_blocks.index(block)] = jnp.zeros((2, 2, 128, 128), jnp.float32)
            else:
                XC[corner_blocks.index(block)] = jnp.zeros((128, 128), jnp.float32)
        pl.when(jnp.logical_not(exists(block)))(clear)

    for copy in small_copies:
        copy.wait()
    live = (LA[1] >= 0).astype(jnp.float32)
    land = LA[0].astype(jnp.float32)

    def spread(values, p, r):
        return jnp.broadcast_to(values[p : p + 1, r : r + 1], (1, 128))

    lives = {(p, r): spread(live, p, r) for p in (0, 1) for r in (0, 1)}
    block_count = lives[0, 0] + lives[0, 1] + lives[1, 0] + lives[1, 1]
    norm = jnp.sqrt(jnp.maximum(block_count, 1.0))
    lane = lax.broadcasted_iota(jnp.int32, (1, 128), 1)
    scalars = jnp.zeros((1, 128), jnp.float32)
    for p in (0, 1):
        for r in (0, 1):
            scalars = jnp.where(lane == 2 * p + r, spread(land, p, r), scalars)
            scalars = jnp.where(lane == 4 + 2 * p + r, lives[p, r] / norm, scalars)

    def mine(field, p, r):
        return SM[own_of[field], p, pl.ds(r, 1), :]

    blank = jnp.zeros((1, 128), jnp.float32)
    head = [scalars, mine("fe", 1, 0), mine("fe", 1, 1), mine("fn", 0, 1), mine("fn", 1, 1)]
    for row, values in enumerate(head + [blank] * 3):
        PK[0, pl.ds(row, 1), :] = values
    for first, field in ((8, "fe"), (12, "fn"), (16, "vd"), (20, "vc")):
        for p in (0, 1):
            for r in (0, 1):
                PK[0, pl.ds(first + 2 * p + r, 1), :] = mine(field, p, r)

    lat_near = jnp.where(inside[1], 1, 0) + jnp.where(inside[-1], 1, 0)
    lat_second = jnp.where(inside[2], 1, 0) + jnp.where(inside[-2], 1, 0)
    from_west = jnp.where(late, 0, 1 + lat_near) + jnp.where(phase > 1, 1, 0)
    awaited_inner = lat_near + lat_second + from_west
    awaited_rim = jnp.where(even, lat_near, 0) + jnp.where(inside[-2], 1, 0)
    pl.semaphore_wait(barrier, 2 + lat_near + jnp.where(rim, awaited_rim, awaited_inner))

    sends = []

    def move(key, source, landing, block):
        place = message[key]
        return pltpu.make_async_remote_copy(
            src_ref=source,
            dst_ref=landing,
            send_sem=send_sem.at[place],
            recv_sem=recv_sem.at[place],
            device_id=target(block),
            device_id_type=MESH,
        )

    def opposite(block):
        return (-block[0], -block[1])

    def packet_ref(block):
        if block in second_blocks:
            return PC.at[second_blocks.index(block)]
        return PK.at[packet_blocks.index(block)]

    def block_ref(cell):
        x, y = cell
        block = (x // 2, y // 2)
        if block in near_blocks:
            return X.at[near_blocks.index(block), x % 2, y % 2]
        return XC.at[corner_blocks.index(block)]

    def block_value(cell):
        x, y = cell
        block = (x // 2, y // 2)
        if block in near_blocks:
            return X[near_blocks.index(block), x % 2, y % 2]
        return XC[corner_blocks.index(block)]

    def corner_of(block):
        p, r = corner_cell(block)
        return (2 * block[0] + p, 2 * block[1] + r)

    listed = set()

    def send(key, source, landing, goal, condition):
        copy = move(key, source, landing, goal)
        only(condition, copy.start)
        if (key, goal) not in listed:
            sends.append((key, goal, exists(goal) if key[0] != "corner" else condition))
            listed.add((key, goal))

    def send_packet(goal, condition=None):
        seen = opposite(goal)
        source = PK.at[0, pl.ds(0, 8)] if seen in second_blocks else PK.at[0]
        send(("packet", seen), source, packet_ref(seen), goal, both(exists(goal), condition))

    def send_blocks(goal, cells, condition=None):
        seen = opposite(goal)
        for cell in cells(seen):
            source = X.at[0, cell[0] % 2, cell[1] % 2]
            send(("block", cell), source, block_ref(cell), goal, both(exists(goal), condition))

    def mate(goal):
        return even if goal == north else odd

    def relay_corners(block):
        for goal in (north, south):
            seen = (block[0], -goal[1])
            cell = corner_of(seen)
            source = block_ref((cell[0], cell[1] + 2 * goal[1]))
            condition = mate(goal) if block == west else exists(goal)
            send(("corner", seen), source, block_ref(cell), goal, condition)

    def send_across(goal, condition):
        seen = opposite(goal)
        cell = corner_of(seen)
        source = X.at[0, cell[0] % 2, cell[1] % 2]
        send(("corner", seen), source, block_ref(cell), goal, condition)

    def wait(key, source, landing, origin, condition):
        only(condition, move(key, source, landing, origin).wait_recv)

    def wait_packet(block, condition=None):
        landing = packet_ref(block)
        source = PK.at[0, pl.ds(0, 8)] if block in second_blocks else PK.at[0]
        wait(("packet", block), source, landing, block, both(exists(block), condition))

    def wait_block(cell):
        block = (cell[0] // 2, cell[1] // 2)
        wait(("block", cell), X.at[0, 0, 0], block_ref(cell), block, exists(block))

    def serve(goal, condition=None):
        for cells in (near_cells, far_cells):
            send_blocks(goal, cells, condition)

    west_side = [west, (-1, 1), (-1, -1)]
    free_west = jnp.logical_and(phase > 0, inner)
    free_second = jnp.logical_and(phase > 1, inner)
    held_lat = jnp.logical_and(rim, odd)
    free_lat = jnp.logical_not(held_lat)
    for goal in (east, (2, 0), (1, 1), (1, -1)):
        send_packet(goal)
    inverse_copy.wait()
    send_across((1, 1), across_up)
    send_across((1, -1), across_down)
    for goal in west_side:
        send_packet(goal, free_west)
    send_packet((-2, 0), free_second)
    send_packet(north, free_lat)
    send_packet(south, free_lat)
    send_packet((0, 2), inner)
    send_packet((0, -2))
    serve(east)
    for cells in (near_cells, far_cells):
        send_blocks(west, cells, free_west)
        send_blocks(north, cells, free_lat)
        send_blocks(south, cells, free_lat)
    for block in (north, south):
        wait_packet(block, held_lat)
        send_packet(block, held_lat)
        serve(block, held_lat)
    for block in [(0, 2)] + west_side:
        wait_packet(block, rim)
        send_packet(block, rim)
    serve(west, rim)
    wait_packet((-2, 0), rim)
    send_packet((-2, 0), rim)

    cache = {}

    def field(name, cell):
        if (name, cell) in cache:
            return cache[name, cell]
        x, y = cell
        block = (x // 2, y // 2)
        p, r = x % 2, y % 2
        place = 2 * p + r
        if block in second_blocks:
            ref, at = PC, second_blocks.index(block)
            row = {"fe": 1 + r, "fn": 3 + p}.get(name, 0)
            assert (name != "fe" or p == 1) and (name != "fn" or r == 1)
        else:
            ref, at = PK, packet_blocks.index(block)
            row = {"fe": 8, "fn": 12, "vd": 16, "vc": 20}.get(name, 0) + place
        if name in ("land", "w"):
            lane_at = place + (4 if name == "w" else 0)
            row_values = ref[at, pl.ds(0, 1), :]
            value = jnp.broadcast_to(row_values[:, lane_at : lane_at + 1], (1, 128))
        else:
            value = ref[at, pl.ds(row, 1), :]
        cache[name, cell] = value
        return value

    def face(low, high):
        if ("face", low, high) not in cache:
            name = "fe" if low[1] == high[1] else "fn"
            cache["face", low, high] = field(name, low) * (field("land", low) * field("land", high))
        return cache["face", low, high]

    def between(cell, other):
        return face(*sorted((cell, other)))

    def coef(cell, row):
        return CF[pl.ds(COEFS * cell_index[cell] + row, 1), :]

    def edge(cell, other):
        return CF[pl.ds(edge_index[tuple(sorted((cell, other)))], 1), :]

    top = lax.broadcasted_iota(jnp.int32, (1, 128), 1) < 127

    def make_coefs(cell):
        x, y = cell
        p, r = x % 2, y % 2
        lon_cross, lon_same = ((x - 1, y), (x + 1, y)) if p == 0 else ((x + 1, y), (x - 1, y))
        lat_cross, lat_same = ((x, y - 1), (x, y + 1)) if r == 0 else ((x, y + 1), (x, y - 1))
        w = field("w", cell)
        vc = field("vc", cell)
        main = field("vd", cell) + vc + down(vc)
        for other in neighbours(cell):
            main = main + between(cell, other)
        same = between(cell, lon_same) * field("w", lon_same)
        same = same + between(cell, lat_same) * field("w", lat_same)
        weighted = w * main - same
        up = jnp.where(top, vc, 0.0)
        below = down(up)
        rows = [
            w,
            -relax * weighted,
            relax * w * below,
            relax * w * up,
            relax * between(cell, lon_cross) * field("w", lon_cross),
            relax * between(cell, lat_cross) * field("w", lat_cross),
        ]
        if cell in support:
            rows += [main, -below, -up]
        for row, values in enumerate(rows):
            CF[pl.ds(COEFS * cell_index[cell] + row, 1), :] = values

    def roll_down(values):
        return pltpu.roll(values, 1, 1)

    def roll_up(values):
        return pltpu.roll(values, 127, 1)

    diagonal = lax.broadcasted_iota(jnp.int32, (128, 128), 0) == lax.broadcasted_iota(
        jnp.int32, (128, 128), 1
    )

    def own_columns(cells):
        for cell in cells:
            inverse = block_value(cell)
            values = jnp.where(diagonal, coef(cell, 0), 0.0) + inverse * coef(cell, 1)
            values = values + roll_down(inverse) * coef(cell, 2) + roll_up(inverse) * coef(cell, 3)
            PT[cell_index[cell]] = values.T

    def near_columns(side):
        for cell in near_cells(side):
            inner = (cell[0] - side[0], cell[1] - side[1])
            scale = relax * between(cell, inner) * field("w", inner)
            PT[cell_index[cell]] = (block_value(cell) * scale).T

    def edges(early):
        for low, high in edge_list:
            if (high[0] >= 0 and low[0] >= 0) == early:
                CF[pl.ds(edge_index[low, high], 1), :] = face(low, high)

    filled = set()

    def add(block, values):
        place = slot_of[block]
        if place in filled:
            out[place] = out[place] + values
        else:
            out[place] = values
            filled.add(place)

    def galerkin(cell):
        x, y = cell
        a, b = x // 2, y // 2
        applied = None
        if cell in support:
            own = PT[cell_index[cell]]
            applied = own * coef(cell, 6) + roll_down(own) * coef(cell, 7) + roll_up(own) * coef(cell, 8)
        for other in neighbours(cell):
            if other in support:
                term = PT[cell_index[other]] * edge(cell, other)
                applied = -term if applied is None else applied - term
        high, low = split(applied)
        left = jnp.concatenate([high, low], axis=1)
        high, low = split(block_value(cell))
        right = jnp.concatenate([high, low], axis=1)
        right = jnp.concatenate([right, right], axis=0)
        product = jnp.dot(left, right, preferred_element_type=jnp.float32)
        product = product[:, :128] + product[:, 128:]
        own = applied * coef(cell, 0) + product * coef(cell, 1)
        own = own + roll_down(product) * coef(cell, 2) + roll_up(product) * coef(cell, 3)
        add((a, b), own)
        add((a + (1 if x % 2 else -1), b), product * coef(cell, 4))
        add((a, b + (1 if y % 2 else -1)), product * coef(cell, 5))

    def corner(block):
        landing = XC.at[corner_blocks.index(block)]
        wait(("corner", block), X.at[0, 0, 0], landing, (0, block[1]), exists(block))
        galerkin(corner_of(block))

    for block in (east, (2, 0), (1, 1), (1, -1), (0, -2)):
        wait_packet(block)
    wait_packet(north, free_lat)
    wait_packet(south, free_lat)
    wait_packet((0, 2), inner)
    for cell in all_cells:
        if cell[0] > 0:
            make_coefs(cell)
    edges(True)
    own_columns(own_cells[2:])
    for side in (north, south, east):
        for cell in near_cells(side):
            wait_block(cell)
        if side == east:
            relay_corners(side)
        near_columns(side)
    for cell in near_cells(east):
        galerkin(cell)
    for side in (north, south):
        galerkin(near_cells(side)[1])
        for cell in far_cells(side):
            wait_block(cell)
        galerkin(far_cells(side)[1])
    for cell in far_cells(east):
        wait_block(cell)
        galerkin(cell)
    for block in corner_blocks:
        if block[0] > 0:
            corner(block)

    for block in west_side + [(-2, 0)]:
        wait_packet(block, inner)
        send_packet(block, phase <= 1 if block == (-2, 0) else late)
    for cell in all_cells:
        if cell[0] <= 0:
            make_coefs(cell)
    edges(False)
    own_columns(own_cells[:2])
    for cell in own_cells[2:]:
        galerkin(cell)
    for side in (north, south):
        for cell in (near_cells(side)[0], far_cells(side)[0]):
            galerkin(cell)
    for cell in near_cells(west):
        wait_block(cell)
    relay_corners(west)
    serve(west, late)
    near_columns(west)
    for cell in own_cells[:2] + near_cells(west):
        galerkin(cell)
    for cell in far_cells(west):
        wait_block(cell)
        galerkin(cell)
    for block in corner_blocks:
        if block[0] < 0:
            corner(block)
    assert len(filled) == len(offsets)
    for key, goal, condition in sends:
        def drain(key=key, goal=goal):
            source = X.at[0, 0, 0]
            if key[0] == "packet":
                source = PK.at[0, pl.ds(0, 8)] if key[1] in second_blocks else PK.at[0]
            move(key, source, source, goal).wait_send()
        only(condition, drain)


def publish(held, out, sem):
    copies = [
        pltpu.make_async_copy(held.at[place], out.at[place], sem.at[place])
        for place in range(len(offsets))
    ]
    for copy in copies:
        copy.start()
    for copy in copies:
        copy.wait()


def local(inverse, vert_diag, vert_coup, face_east, face_north, land_mask, aggregate):
    blocks = len(offsets)
    messages = len(message)
    anywhere = pl.BlockSpec(memory_space=pltpu.HBM)
    held = pl.pallas_call(
        kernel,
        out_shape=pltpu.VMEM((blocks, 128, 128), jnp.float32),
        in_specs=[anywhere] * 7,
        out_specs=pl.BlockSpec(memory_space=pltpu.VMEM),
        scratch_shapes=[
            pltpu.VMEM((5, 2, 2, 128, 128), jnp.float32),
            pltpu.VMEM((4, 128, 128), jnp.float32),
            pltpu.VMEM((9, 24, 128), jnp.float32),
            pltpu.VMEM((4, 8, 128), jnp.float32),
            pltpu.VMEM((4, 2, 2, 128), jnp.float32),
            pltpu.VMEM((2, 2, 2), jnp.int32),
            pltpu.VMEM((len(support), 128, 128), jnp.float32),
            pltpu.VMEM((coef_rows, 128), jnp.float32),
            pltpu.SemaphoreType.DMA((7,)),
            pltpu.SemaphoreType.DMA((messages,)),
            pltpu.SemaphoreType.DMA((messages,)),
        ],
        compiler_params=pltpu.CompilerParams(collective_id=0, has_side_effects=True),
    )(inverse, vert_diag, vert_coup, face_east, face_north, land_mask, aggregate)
    coarse = pl.pallas_call(
        publish,
        out_shape=jax.ShapeDtypeStruct((blocks, 128, 128), jnp.float32),
        in_specs=[pl.BlockSpec(memory_space=pltpu.VMEM)],
        out_specs=anywhere,
        scratch_shapes=[pltpu.SemaphoreType.DMA((blocks,))],
        compiler_params=pltpu.CompilerParams(vmem_limit_bytes=2**20),
    )(held)
    return coarse[None, None]


def solution(mesh):
    return jax.shard_map(
        local,
        mesh=mesh,
        in_specs=(
            P("lon", "lat", None, None),
            P("lon", "lat", None),
            P("lon", "lat", None),
            P("lon", "lat", None),
            P("lon", "lat", None),
            P("lon", "lat"),
            P("lon", "lat"),
        ),
        out_specs=P("lon", "lat", None, None, None),
        check_vma=False,
    )
```

```python
import jax
import jax.numpy as jnp
from jax import lax
from jax.experimental import pallas as pl
from jax.experimental.pallas import tpu as pltpu
from jax.sharding import PartitionSpec as P

MESH = pl.DeviceIdType.MESH
relax = 0.6
offsets = [
    (-2, 0),
    (-1, -1),
    (-1, 0),
    (-1, 1),
    (0, -2),
    (0, -1),
    (0, 0),
    (0, 1),
    (0, 2),
    (1, -1),
    (1, 0),
    (1, 1),
    (2, 0),
]
slot_of = {offset: place for place, offset in enumerate(offsets)}
near_blocks = [(0, 0), (1, 0), (-1, 0), (0, 1), (0, -1)]
second_blocks = [(2, 0), (-2, 0), (0, 2), (0, -2)]
corner_blocks = [(1, 1), (-1, 1), (1, -1), (-1, -1)]
packet_blocks = near_blocks + corner_blocks
sides = [(1, 0), (-1, 0), (0, 1), (0, -1)]


def corner_cell(block):
    return (0 if block[0] > 0 else 1, 0 if block[1] > 0 else 1)


def cells_of(block):
    return [(2 * block[0] + p, 2 * block[1] + r) for p in (0, 1) for r in (0, 1)]


def near_cells(side):
    a, b = side
    if b == 0:
        p = 0 if a > 0 else 1
        return [(2 * a + p, r) for r in (0, 1)]
    r = 0 if b > 0 else 1
    return [(p, 2 * b + r) for p in (0, 1)]


def far_cells(side):
    near = near_cells(side)
    return [cell for cell in cells_of(side) if cell not in near]


def neighbours(cell):
    x, y = cell
    return [(x + 1, y), (x - 1, y), (x, y + 1), (x, y - 1)]


own_cells = cells_of((0, 0))
support = own_cells + [cell for side in sides for cell in near_cells(side)]
outer = [cell for side in sides for cell in far_cells(side)] + [
    (2 * a + corner_cell((a, b))[0], 2 * b + corner_cell((a, b))[1]) for a, b in corner_blocks
]
all_cells = support + outer
cell_index = {cell: place for place, cell in enumerate(all_cells)}
COEFS = 9
edge_list = []
for cell in support:
    for other in neighbours(cell):
        key = tuple(sorted((cell, other)))
        if key not in edge_list:
            edge_list.append(key)
edge_index = {edge: COEFS * len(all_cells) + place for place, edge in enumerate(edge_list)}
coef_rows = COEFS * len(all_cells) + len(edge_list)
coef_rows = (coef_rows + 7) // 8 * 8

message = {}
for block in near_blocks[1:] + second_blocks + corner_blocks:
    message["packet", block] = len(message)
for side in sides:
    for cell in near_cells(side) + far_cells(side):
        message["block", cell] = len(message)
for block in corner_blocks:
    message["corner", block] = len(message)


def down(values):
    lane = lax.broadcasted_iota(jnp.int32, values.shape, 1)
    return jnp.where(lane > 0, pltpu.roll(values, 1, 1), 0.0)


def split(values):
    high = values.astype(jnp.bfloat16)
    low = (values - high.astype(jnp.float32)).astype(jnp.bfloat16)
    return high, low


def kernel(
    inv_h, vd_h, vc_h, fe_h, fn_h, land_h, agg_h,
    out,
    X, XC, PK, PC, SM, LA, PT, CF,
    local_sem, send_sem, recv_sem,
):
    me_lon = lax.axis_index("lon")
    me_lat = lax.axis_index("lat")
    count_lon = lax.axis_size("lon")
    count_lat = lax.axis_size("lat")
    own_of = {"vd": 0, "vc": 1, "fe": 2, "fn": 3}
    east, west, north, south = sides

    small_copies = [
        pltpu.make_async_copy(source, SM.at[place], local_sem.at[1 + place])
        for place, source in enumerate((vd_h, vc_h, fe_h, fn_h))
    ] + [
        pltpu.make_async_copy(source, LA.at[place], local_sem.at[5 + place])
        for place, source in enumerate((land_h, agg_h))
    ]
    inverse_copy = pltpu.make_async_copy(inv_h, X.at[0], local_sem.at[0])
    for copy in small_copies:
        copy.start()
    inverse_copy.start()

    def target(block):
        a, b = block
        return {"lon": lax.rem(me_lon + a + count_lon, count_lon), "lat": me_lat + b}

    inside = {b: me_lat + b < count_lat if b > 0 else me_lat + b >= 0 for b in (-2, -1, 1, 2)}

    def exists(block):
        return inside.get(block[1])

    def both(first, second):
        if first is None:
            return second
        return first if second is None else jnp.logical_and(first, second)

    def only(condition, action):
        if condition is None:
            action()
        else:
            pl.when(condition)(action)

    phase = lax.rem(me_lon, 64)
    late = phase == 0
    rim = phase == 63
    inner = phase < 63
    even = lax.rem(me_lat, 2) == 0
    odd = lax.rem(me_lat, 2) == 1
    across_up = jnp.logical_and(odd, me_lat + 1 < count_lat)
    across_down = jnp.logical_and(even, me_lat >= 1)
    barrier = pltpu.get_barrier_semaphore()
    for block in near_blocks[1:] + second_blocks + corner_blocks:
        reach = None
        if block[0] > 0:
            reach = phase < 63 - block[0]
        elif block == (0, 1):
            reach = jnp.logical_or(inner, odd)
        elif block == (0, -1):
            reach = jnp.logical_or(inner, odd)
        elif block == (0, -2):
            reach = inner
        def signal(block=block):
            pl.semaphore_signal(barrier, inc=1, device_id=target(block), device_id_type=MESH)
        only(both(exists(block), reach), signal)

    partners = near_blocks[1:] + second_blocks + corner_blocks
    for block in partners:
        if block[1] == 0:
            continue
        def clear(block=block):
            if block in second_blocks:
                PC[second_blocks.index(block)] = jnp.zeros((8, 128), jnp.float32)
                return
            PK[packet_blocks.index(block)] = jnp.zeros((24, 128), jnp.float32)
            if block in near_blocks:
                X[near_blocks.index(block)] = jnp.zeros((2, 2, 128, 128), jnp.float32)
            else:
                XC[corner_blocks.index(block)] = jnp.zeros((128, 128), jnp.float32)
        pl.when(jnp.logical_not(exists(block)))(clear)

    for copy in small_copies:
        copy.wait()
    live = (LA[1] >= 0).astype(jnp.float32)
    land = LA[0].astype(jnp.float32)

    def spread(values, p, r):
        return jnp.broadcast_to(values[p : p + 1, r : r + 1], (1, 128))

    lives = {(p, r): spread(live, p, r) for p in (0, 1) for r in (0, 1)}
    block_count = lives[0, 0] + lives[0, 1] + lives[1, 0] + lives[1, 1]
    norm = jnp.sqrt(jnp.maximum(block_count, 1.0))
    lane = lax.broadcasted_iota(jnp.int32, (1, 128), 1)
    scalars = jnp.zeros((1, 128), jnp.float32)
    for p in (0, 1):
        for r in (0, 1):
            scalars = jnp.where(lane == 2 * p + r, spread(land, p, r), scalars)
            scalars = jnp.where(lane == 4 + 2 * p + r, lives[p, r] / norm, scalars)

    def mine(field, p, r):
        return SM[own_of[field], p, pl.ds(r, 1), :]

    blank = jnp.zeros((1, 128), jnp.float32)
    head = [scalars, mine("fe", 1, 0), mine("fe", 1, 1), mine("fn", 0, 1), mine("fn", 1, 1)]
    for row, values in enumerate(head + [blank] * 3):
        PK[0, pl.ds(row, 1), :] = values
    for first, field in ((8, "fe"), (12, "fn"), (16, "vd"), (20, "vc")):
        for p in (0, 1):
            for r in (0, 1):
                PK[0, pl.ds(first + 2 * p + r, 1), :] = mine(field, p, r)

    lat_near = jnp.where(inside[1], 1, 0) + jnp.where(inside[-1], 1, 0)
    lat_second = jnp.where(inside[2], 1, 0) + jnp.where(inside[-2], 1, 0)
    from_west = jnp.where(late, 0, 1 + lat_near) + jnp.where(phase > 1, 1, 0)
    awaited_inner = lat_near + lat_second + from_west
    awaited_rim = jnp.where(even, lat_near, 0) + jnp.where(inside[-2], 1, 0)
    pl.semaphore_wait(barrier, 2 + lat_near + jnp.where(rim, awaited_rim, awaited_inner))

    sends = []

    def move(key, source, landing, block):
        place = message[key]
        return pltpu.make_async_remote_copy(
            src_ref=source,
            dst_ref=landing,
            send_sem=send_sem.at[place],
            recv_sem=recv_sem.at[place],
            device_id=target(block),
            device_id_type=MESH,
        )

    def opposite(block):
        return (-block[0], -block[1])

    def packet_ref(block):
        if block in second_blocks:
            return PC.at[second_blocks.index(block)]
        return PK.at[packet_blocks.index(block)]

    def block_ref(cell):
        x, y = cell
        block = (x // 2, y // 2)
        if block in near_blocks:
            return X.at[near_blocks.index(block), x % 2, y % 2]
        return XC.at[corner_blocks.index(block)]

    def block_value(cell):
        x, y = cell
        block = (x // 2, y // 2)
        if block in near_blocks:
            return X[near_blocks.index(block), x % 2, y % 2]
        return XC[corner_blocks.index(block)]

    def corner_of(block):
        p, r = corner_cell(block)
        return (2 * block[0] + p, 2 * block[1] + r)

    listed = set()
    drains = {}

    def send(key, source, landing, goal, condition):
        copy = move(key, source, landing, goal)
        only(condition, copy.start)
        if (key, goal) not in listed:
            sends.append((key, goal))
            listed.add((key, goal))

    def send_packet(goal, condition=None):
        seen = opposite(goal)
        source = PK.at[0, pl.ds(0, 8)] if seen in second_blocks else PK.at[0]
        send(("packet", seen), source, packet_ref(seen), goal, both(exists(goal), condition))

    def send_blocks(goal, cells, condition=None):
        seen = opposite(goal)
        for cell in cells(seen):
            source = X.at[0, cell[0] % 2, cell[1] % 2]
            send(("block", cell), source, block_ref(cell), goal, both(exists(goal), condition))

    def pass_near(side, condition=None):
        for cell in near_cells(side):
            wait_block(cell, condition)
            if side in (east, west):
                goal = north if cell[1] else south
                seen = (side[0], -goal[1])
                landing = block_ref(corner_of(seen))
                facing = exists(goal)
                if side == west:
                    facing = even if goal == north else odd
                send(("corner", seen), block_ref(cell), landing, goal, both(facing, condition))
                drains["corner", seen, goal] = facing

    def send_across(goal, condition):
        seen = opposite(goal)
        cell = corner_of(seen)
        source = X.at[0, cell[0] % 2, cell[1] % 2]
        send(("corner", seen), source, block_ref(cell), goal, condition)
        drains["corner", seen, goal] = condition

    def wait(key, source, landing, origin, condition):
        only(condition, move(key, source, landing, origin).wait_recv)

    def wait_packet(block, condition=None):
        landing = packet_ref(block)
        source = PK.at[0, pl.ds(0, 8)] if block in second_blocks else PK.at[0]
        wait(("packet", block), source, landing, block, both(exists(block), condition))

    def wait_block(cell, condition=None):
        block = (cell[0] // 2, cell[1] // 2)
        arrived = both(exists(block), condition)
        wait(("block", cell), X.at[0, 0, 0], block_ref(cell), block, arrived)

    def serve(goal, condition=None):
        for cells in (near_cells, far_cells):
            send_blocks(goal, cells, condition)

    west_side = [west, (-1, 1), (-1, -1)]
    free_west = jnp.logical_and(phase > 0, inner)
    free_second = jnp.logical_and(phase > 1, inner)
    held_lat = jnp.logical_and(rim, odd)
    free_lat = jnp.logical_not(held_lat)
    for goal in (east, (2, 0), (1, 1), (1, -1)):
        send_packet(goal)
    inverse_copy.wait()
    send_across((1, 1), across_up)
    send_across((1, -1), across_down)
    for goal in west_side:
        send_packet(goal, free_west)
    send_packet((-2, 0), free_second)
    send_packet(north, free_lat)
    send_packet(south, free_lat)
    send_packet((0, 2), inner)
    send_packet((0, -2))
    serve(east)
    for cells in (near_cells, far_cells):
        send_blocks(west, cells, free_west)
        send_blocks(north, cells, free_lat)
        send_blocks(south, cells, free_lat)
    for block in (north, south):
        wait_packet(block, held_lat)
        send_packet(block, held_lat)
        serve(block, held_lat)
    for block in [(0, 2)] + west_side:
        wait_packet(block, rim)
        send_packet(block, rim)
    serve(west, rim)
    wait_packet((-2, 0), rim)
    send_packet((-2, 0), rim)

    cache = {}

    def field(name, cell):
        if (name, cell) in cache:
            return cache[name, cell]
        x, y = cell
        block = (x // 2, y // 2)
        p, r = x % 2, y % 2
        place = 2 * p + r
        if block in second_blocks:
            ref, at = PC, second_blocks.index(block)
            row = {"fe": 1 + r, "fn": 3 + p}.get(name, 0)
            assert (name != "fe" or p == 1) and (name != "fn" or r == 1)
        else:
            ref, at = PK, packet_blocks.index(block)
            row = {"fe": 8, "fn": 12, "vd": 16, "vc": 20}.get(name, 0) + place
        if name in ("land", "w"):
            lane_at = place + (4 if name == "w" else 0)
            row_values = ref[at, pl.ds(0, 1), :]
            value = jnp.broadcast_to(row_values[:, lane_at : lane_at + 1], (1, 128))
        else:
            value = ref[at, pl.ds(row, 1), :]
        cache[name, cell] = value
        return value

    def face(low, high):
        if ("face", low, high) not in cache:
            name = "fe" if low[1] == high[1] else "fn"
            cache["face", low, high] = field(name, low) * (field("land", low) * field("land", high))
        return cache["face", low, high]

    def between(cell, other):
        return face(*sorted((cell, other)))

    def coef(cell, row):
        return CF[pl.ds(COEFS * cell_index[cell] + row, 1), :]

    def edge(cell, other):
        return CF[pl.ds(edge_index[tuple(sorted((cell, other)))], 1), :]

    top = lax.broadcasted_iota(jnp.int32, (1, 128), 1) < 127

    def make_coefs(cell):
        x, y = cell
        p, r = x % 2, y % 2
        lon_cross, lon_same = ((x - 1, y), (x + 1, y)) if p == 0 else ((x + 1, y), (x - 1, y))
        lat_cross, lat_same = ((x, y - 1), (x, y + 1)) if r == 0 else ((x, y + 1), (x, y - 1))
        w = field("w", cell)
        vc = field("vc", cell)
        main = field("vd", cell) + vc + down(vc)
        for other in neighbours(cell):
            main = main + between(cell, other)
        same = between(cell, lon_same) * field("w", lon_same)
        same = same + between(cell, lat_same) * field("w", lat_same)
        weighted = w * main - same
        up = jnp.where(top, vc, 0.0)
        below = down(up)
        rows = [
            w,
            -relax * weighted,
            relax * w * below,
            relax * w * up,
            relax * between(cell, lon_cross) * field("w", lon_cross),
            relax * between(cell, lat_cross) * field("w", lat_cross),
        ]
        if cell in support:
            rows += [main, -below, -up]
        for row, values in enumerate(rows):
            CF[pl.ds(COEFS * cell_index[cell] + row, 1), :] = values

    def roll_down(values):
        return pltpu.roll(values, 1, 1)

    def roll_up(values):
        return pltpu.roll(values, 127, 1)

    diagonal = lax.broadcasted_iota(jnp.int32, (128, 128), 0) == lax.broadcasted_iota(
        jnp.int32, (128, 128), 1
    )

    def own_columns(cells):
        for cell in cells:
            inverse = block_value(cell)
            values = jnp.where(diagonal, coef(cell, 0), 0.0) + inverse * coef(cell, 1)
            values = values + roll_down(inverse) * coef(cell, 2) + roll_up(inverse) * coef(cell, 3)
            PT[cell_index[cell]] = values.T

    def near_columns(side):
        for cell in near_cells(side):
            inner = (cell[0] - side[0], cell[1] - side[1])
            scale = relax * between(cell, inner) * field("w", inner)
            PT[cell_index[cell]] = (block_value(cell) * scale).T

    def edges(early):
        for low, high in edge_list:
            if (high[0] >= 0 and low[0] >= 0) == early:
                CF[pl.ds(edge_index[low, high], 1), :] = face(low, high)

    filled = set()

    def add(block, values):
        place = slot_of[block]
        if place in filled:
            out[place] = out[place] + values
        else:
            out[place] = values
            filled.add(place)

    def galerkin(cell):
        x, y = cell
        a, b = x // 2, y // 2
        applied = None
        if cell in support:
            own = PT[cell_index[cell]]
            applied = own * coef(cell, 6) + roll_down(own) * coef(cell, 7) + roll_up(own) * coef(cell, 8)
        for other in neighbours(cell):
            if other in support:
                term = PT[cell_index[other]] * edge(cell, other)
                applied = -term if applied is None else applied - term
        high, low = split(applied)
        left = jnp.concatenate([high, low], axis=1)
        high, low = split(block_value(cell))
        right = jnp.concatenate([high, low], axis=1)
        right = jnp.concatenate([right, right], axis=0)
        product = jnp.dot(left, right, preferred_element_type=jnp.float32)
        product = product[:, :128] + product[:, 128:]
        own = applied * coef(cell, 0) + product * coef(cell, 1)
        own = own + roll_down(product) * coef(cell, 2) + roll_up(product) * coef(cell, 3)
        add((a, b), own)
        add((a + (1 if x % 2 else -1), b), product * coef(cell, 4))
        add((a, b + (1 if y % 2 else -1)), product * coef(cell, 5))

    def corner(block):
        landing = XC.at[corner_blocks.index(block)]
        wait(("corner", block), X.at[0, 0, 0], landing, (0, block[1]), exists(block))
        galerkin(corner_of(block))

    for block in (east, (2, 0), (1, 1), (1, -1), (0, -2)):
        wait_packet(block)
    wait_packet(north, free_lat)
    wait_packet(south, free_lat)
    wait_packet((0, 2), inner)
    for cell in all_cells:
        if cell[0] > 0:
            make_coefs(cell)
    edges(True)
    own_columns(own_cells[2:])
    pass_near(west, jnp.logical_not(late))
    for side in (east, north, south):
        pass_near(side)
        near_columns(side)
    for cell in near_cells(east):
        galerkin(cell)
    for side in (north, south):
        galerkin(near_cells(side)[1])
        for cell in far_cells(side):
            wait_block(cell)
        galerkin(far_cells(side)[1])
    for cell in far_cells(east):
        wait_block(cell)
        galerkin(cell)
    for block in corner_blocks:
        if block[0] > 0:
            corner(block)

    for block in west_side + [(-2, 0)]:
        wait_packet(block, inner)
        send_packet(block, phase <= 1 if block == (-2, 0) else late)
        if block == west:
            send_blocks(west, near_cells, late)
    for cell in all_cells:
        if cell[0] <= 0:
            make_coefs(cell)
    edges(False)
    own_columns(own_cells[:2])
    for cell in own_cells[2:]:
        galerkin(cell)
    for side in (north, south):
        for cell in (near_cells(side)[0], far_cells(side)[0]):
            galerkin(cell)
    pass_near(west, late)
    send_blocks(west, far_cells, late)
    near_columns(west)
    for cell in own_cells[:2] + near_cells(west):
        galerkin(cell)
    for cell in far_cells(west):
        wait_block(cell)
        galerkin(cell)
    for block in corner_blocks:
        if block[0] < 0:
            corner(block)
    assert len(filled) == len(offsets)
    for key, goal in sends:
        def drain(key=key, goal=goal):
            source = X.at[0, 0, 0]
            if key[0] == "packet":
                source = PK.at[0, pl.ds(0, 8)] if key[1] in second_blocks else PK.at[0]
            move(key, source, source, goal).wait_send()
        only(drains.get(key + (goal,), exists(goal)), drain)


def publish(held, out, sem):
    copies = [
        pltpu.make_async_copy(held.at[place], out.at[place], sem.at[place])
        for place in range(len(offsets))
    ]
    for copy in copies:
        copy.start()
    for copy in copies:
        copy.wait()


def local(inverse, vert_diag, vert_coup, face_east, face_north, land_mask, aggregate):
    blocks = len(offsets)
    messages = len(message)
    anywhere = pl.BlockSpec(memory_space=pltpu.HBM)
    held = pl.pallas_call(
        kernel,
        out_shape=pltpu.VMEM((blocks, 128, 128), jnp.float32),
        in_specs=[anywhere] * 7,
        out_specs=pl.BlockSpec(memory_space=pltpu.VMEM),
        scratch_shapes=[
            pltpu.VMEM((5, 2, 2, 128, 128), jnp.float32),
            pltpu.VMEM((4, 128, 128), jnp.float32),
            pltpu.VMEM((9, 24, 128), jnp.float32),
            pltpu.VMEM((4, 8, 128), jnp.float32),
            pltpu.VMEM((4, 2, 2, 128), jnp.float32),
            pltpu.VMEM((2, 2, 2), jnp.int32),
            pltpu.VMEM((len(support), 128, 128), jnp.float32),
            pltpu.VMEM((coef_rows, 128), jnp.float32),
            pltpu.SemaphoreType.DMA((7,)),
            pltpu.SemaphoreType.DMA((messages,)),
            pltpu.SemaphoreType.DMA((messages,)),
        ],
        compiler_params=pltpu.CompilerParams(collective_id=0, has_side_effects=True),
    )(inverse, vert_diag, vert_coup, face_east, face_north, land_mask, aggregate)
    coarse = pl.pallas_call(
        publish,
        out_shape=jax.ShapeDtypeStruct((blocks, 128, 128), jnp.float32),
        in_specs=[pl.BlockSpec(memory_space=pltpu.VMEM)],
        out_specs=anywhere,
        scratch_shapes=[pltpu.SemaphoreType.DMA((blocks,))],
        compiler_params=pltpu.CompilerParams(vmem_limit_bytes=2**20),
    )(held)
    return coarse[None, None]


def solution(mesh):
    return jax.shard_map(
        local,
        mesh=mesh,
        in_specs=(
            P("lon", "lat", None, None),
            P("lon", "lat", None),
            P("lon", "lat", None),
            P("lon", "lat", None),
            P("lon", "lat", None),
            P("lon", "lat"),
            P("lon", "lat"),
        ),
        out_specs=P("lon", "lat", None, None, None),
        check_vma=False,
    )
```

```python
import jax
import jax.numpy as jnp
from jax import lax
from jax.experimental import pallas as pl
from jax.experimental.pallas import tpu as pltpu
from jax.sharding import PartitionSpec as P

MESH = pl.DeviceIdType.MESH
relax = 0.6
offsets = [
    (-2, 0),
    (-1, -1),
    (-1, 0),
    (-1, 1),
    (0, -2),
    (0, -1),
    (0, 0),
    (0, 1),
    (0, 2),
    (1, -1),
    (1, 0),
    (1, 1),
    (2, 0),
]
slot_of = {offset: place for place, offset in enumerate(offsets)}
near_blocks = [(0, 0), (1, 0), (-1, 0), (0, 1), (0, -1)]
second_blocks = [(2, 0), (-2, 0), (0, 2), (0, -2)]
corner_blocks = [(1, 1), (-1, 1), (1, -1), (-1, -1)]
packet_blocks = near_blocks + corner_blocks
sides = [(1, 0), (-1, 0), (0, 1), (0, -1)]


def corner_cell(block):
    return (0 if block[0] > 0 else 1, 0 if block[1] > 0 else 1)


def cells_of(block):
    return [(2 * block[0] + p, 2 * block[1] + r) for p in (0, 1) for r in (0, 1)]


def near_cells(side):
    a, b = side
    if b == 0:
        p = 0 if a > 0 else 1
        return [(2 * a + p, r) for r in (0, 1)]
    r = 0 if b > 0 else 1
    return [(p, 2 * b + r) for p in (0, 1)]


def far_cells(side):
    near = near_cells(side)
    return [cell for cell in cells_of(side) if cell not in near]


def neighbours(cell):
    x, y = cell
    return [(x + 1, y), (x - 1, y), (x, y + 1), (x, y - 1)]


own_cells = cells_of((0, 0))
support = own_cells + [cell for side in sides for cell in near_cells(side)]
outer = [cell for side in sides for cell in far_cells(side)] + [
    (2 * a + corner_cell((a, b))[0], 2 * b + corner_cell((a, b))[1]) for a, b in corner_blocks
]
all_cells = support + outer
cell_index = {cell: place for place, cell in enumerate(all_cells)}
COEFS = 9
edge_list = []
for cell in support:
    for other in neighbours(cell):
        key = tuple(sorted((cell, other)))
        if key not in edge_list:
            edge_list.append(key)
edge_index = {edge: COEFS * len(all_cells) + place for place, edge in enumerate(edge_list)}
coef_rows = COEFS * len(all_cells) + len(edge_list)
coef_rows = (coef_rows + 7) // 8 * 8

message = {}
for block in near_blocks[1:] + second_blocks + corner_blocks:
    message["packet", block] = len(message)
for side in sides:
    for cell in near_cells(side) + far_cells(side):
        message["block", cell] = len(message)
for block in corner_blocks:
    message["corner", block] = len(message)


def down(values):
    lane = lax.broadcasted_iota(jnp.int32, values.shape, 1)
    return jnp.where(lane > 0, pltpu.roll(values, 1, 1), 0.0)


def split(values):
    high = values.astype(jnp.bfloat16)
    low = (values - high.astype(jnp.float32)).astype(jnp.bfloat16)
    return high, low


def kernel(
    inv_h, vd_h, vc_h, fe_h, fn_h, land_h, agg_h,
    out,
    X, XC, PK, PC, SM, LA, PT, CF,
    local_sem, send_sem, recv_sem,
):
    me_lon = lax.axis_index("lon")
    me_lat = lax.axis_index("lat")
    count_lon = lax.axis_size("lon")
    count_lat = lax.axis_size("lat")
    own_of = {"vd": 0, "vc": 1, "fe": 2, "fn": 3}
    east, west, north, south = sides

    small_copies = [
        pltpu.make_async_copy(source, SM.at[place], local_sem.at[1 + place])
        for place, source in enumerate((vd_h, vc_h, fe_h, fn_h))
    ] + [
        pltpu.make_async_copy(source, LA.at[place], local_sem.at[5 + place])
        for place, source in enumerate((land_h, agg_h))
    ]
    inverse_copy = pltpu.make_async_copy(inv_h, X.at[0], local_sem.at[0])
    for copy in small_copies:
        copy.start()
    inverse_copy.start()

    def target(block):
        a, b = block
        return {"lon": lax.rem(me_lon + a + count_lon, count_lon), "lat": me_lat + b}

    inside = {b: me_lat + b < count_lat if b > 0 else me_lat + b >= 0 for b in (-2, -1, 1, 2)}

    def exists(block):
        return inside.get(block[1])

    def both(first, second):
        if first is None:
            return second
        return first if second is None else jnp.logical_and(first, second)

    def only(condition, action):
        if condition is None:
            action()
        else:
            pl.when(condition)(action)

    phase = lax.rem(me_lon, 64)
    late = phase == 0
    rim = phase == 63
    inner = phase < 63
    even = lax.rem(me_lat, 2) == 0
    odd = lax.rem(me_lat, 2) == 1
    across_up = jnp.logical_and(odd, me_lat + 1 < count_lat)
    across_down = jnp.logical_and(even, me_lat >= 1)
    barrier = pltpu.get_barrier_semaphore()
    for block in near_blocks[1:] + second_blocks + corner_blocks:
        reach = None
        if block[0] > 0:
            reach = phase < 63 - block[0]
        elif block == (0, 1):
            reach = jnp.logical_or(inner, odd)
        elif block == (0, -1):
            reach = jnp.logical_or(inner, odd)
        elif block == (0, -2):
            reach = inner
        def signal(block=block):
            pl.semaphore_signal(barrier, inc=1, device_id=target(block), device_id_type=MESH)
        only(both(exists(block), reach), signal)

    partners = near_blocks[1:] + second_blocks + corner_blocks
    for block in partners:
        if block[1] == 0:
            continue
        def clear(block=block):
            if block in second_blocks:
                PC[second_blocks.index(block)] = jnp.zeros((8, 128), jnp.float32)
                return
            PK[packet_blocks.index(block)] = jnp.zeros((24, 128), jnp.float32)
            if block in near_blocks:
                X[near_blocks.index(block)] = jnp.zeros((2, 2, 128, 128), jnp.float32)
            else:
                XC[corner_blocks.index(block)] = jnp.zeros((128, 128), jnp.float32)
        pl.when(jnp.logical_not(exists(block)))(clear)

    for copy in small_copies:
        copy.wait()
    live = (LA[1] >= 0).astype(jnp.float32)
    land = LA[0].astype(jnp.float32)

    def spread(values, p, r):
        return jnp.broadcast_to(values[p : p + 1, r : r + 1], (1, 128))

    lives = {(p, r): spread(live, p, r) for p in (0, 1) for r in (0, 1)}
    block_count = lives[0, 0] + lives[0, 1] + lives[1, 0] + lives[1, 1]
    norm = jnp.sqrt(jnp.maximum(block_count, 1.0))
    lane = lax.broadcasted_iota(jnp.int32, (1, 128), 1)
    scalars = jnp.zeros((1, 128), jnp.float32)
    for p in (0, 1):
        for r in (0, 1):
            scalars = jnp.where(lane == 2 * p + r, spread(land, p, r), scalars)
            scalars = jnp.where(lane == 4 + 2 * p + r, lives[p, r] / norm, scalars)

    def mine(field, p, r):
        return SM[own_of[field], p, pl.ds(r, 1), :]

    blank = jnp.zeros((1, 128), jnp.float32)
    head = [scalars, mine("fe", 1, 0), mine("fe", 1, 1), mine("fn", 0, 1), mine("fn", 1, 1)]
    for row, values in enumerate(head + [blank] * 3):
        PK[0, pl.ds(row, 1), :] = values
    for first, field in ((8, "fe"), (12, "fn"), (16, "vd"), (20, "vc")):
        for p in (0, 1):
            for r in (0, 1):
                PK[0, pl.ds(first + 2 * p + r, 1), :] = mine(field, p, r)

    lat_near = jnp.where(inside[1], 1, 0) + jnp.where(inside[-1], 1, 0)
    lat_second = jnp.where(inside[2], 1, 0) + jnp.where(inside[-2], 1, 0)
    from_west = jnp.where(late, 0, 1 + lat_near) + jnp.where(phase > 1, 1, 0)
    awaited_inner = lat_near + lat_second + from_west
    awaited_rim = jnp.where(even, lat_near, 0) + jnp.where(inside[-2], 1, 0)
    pl.semaphore_wait(barrier, 2 + lat_near + jnp.where(rim, awaited_rim, awaited_inner))

    sends = []

    def move(key, source, landing, block):
        place = message[key]
        return pltpu.make_async_remote_copy(
            src_ref=source,
            dst_ref=landing,
            send_sem=send_sem.at[place],
            recv_sem=recv_sem.at[place],
            device_id=target(block),
            device_id_type=MESH,
        )

    def opposite(block):
        return (-block[0], -block[1])

    def packet_ref(block):
        if block in second_blocks:
            return PC.at[second_blocks.index(block)]
        return PK.at[packet_blocks.index(block)]

    def block_ref(cell):
        x, y = cell
        block = (x // 2, y // 2)
        if block in near_blocks:
            return X.at[near_blocks.index(block), x % 2, y % 2]
        return XC.at[corner_blocks.index(block)]

    def block_value(cell):
        x, y = cell
        block = (x // 2, y // 2)
        if block in near_blocks:
            return X[near_blocks.index(block), x % 2, y % 2]
        return XC[corner_blocks.index(block)]

    def corner_of(block):
        p, r = corner_cell(block)
        return (2 * block[0] + p, 2 * block[1] + r)

    listed = set()
    drains = {}

    def send(key, source, landing, goal, condition):
        copy = move(key, source, landing, goal)
        only(condition, copy.start)
        if (key, goal) not in listed:
            sends.append((key, goal))
            listed.add((key, goal))

    def send_packet(goal, condition=None):
        seen = opposite(goal)
        source = PK.at[0, pl.ds(0, 8)] if seen in second_blocks else PK.at[0]
        send(("packet", seen), source, packet_ref(seen), goal, both(exists(goal), condition))

    def send_blocks(goal, cells, condition=None):
        seen = opposite(goal)
        for cell in cells(seen):
            source = X.at[0, cell[0] % 2, cell[1] % 2]
            send(("block", cell), source, block_ref(cell), goal, both(exists(goal), condition))

    def pass_block(side, cell, condition):
        wait_block(cell, condition)
        if side not in (east, west):
            return
        goal = north if cell[1] else south
        seen = (side[0], -goal[1])
        landing = block_ref(corner_of(seen))
        facing = exists(goal)
        if side == west:
            facing = even if goal == north else odd
        send(("corner", seen), block_ref(cell), landing, goal, both(facing, condition))
        drains["corner", seen, goal] = facing

    def pass_near(side, condition=None):
        first, second = near_cells(side)
        if side == west:
            pass_block(side, second, both(condition, even))
            pass_block(side, first, condition)
            pass_block(side, second, both(condition, odd))
        else:
            pass_block(side, first, condition)
            pass_block(side, second, condition)

    def send_across(goal, condition):
        seen = opposite(goal)
        cell = corner_of(seen)
        source = X.at[0, cell[0] % 2, cell[1] % 2]
        send(("corner", seen), source, block_ref(cell), goal, condition)
        drains["corner", seen, goal] = condition

    def wait(key, source, landing, origin, condition):
        only(condition, move(key, source, landing, origin).wait_recv)

    def wait_packet(block, condition=None):
        landing = packet_ref(block)
        source = PK.at[0, pl.ds(0, 8)] if block in second_blocks else PK.at[0]
        wait(("packet", block), source, landing, block, both(exists(block), condition))

    def wait_block(cell, condition=None):
        block = (cell[0] // 2, cell[1] // 2)
        arrived = both(exists(block), condition)
        wait(("block", cell), X.at[0, 0, 0], block_ref(cell), block, arrived)

    def serve(goal, condition=None):
        for cells in (near_cells, far_cells):
            send_blocks(goal, cells, condition)

    west_side = [west, (-1, 1), (-1, -1)]
    free_west = jnp.logical_and(phase > 0, inner)
    free_second = jnp.logical_and(phase > 1, inner)
    held_lat = jnp.logical_and(rim, odd)
    free_lat = jnp.logical_not(held_lat)
    for goal in (east, (2, 0), (1, 1), (1, -1)):
        send_packet(goal)
    inverse_copy.wait()
    send_across((1, 1), across_up)
    send_across((1, -1), across_down)
    for goal in west_side:
        send_packet(goal, free_west)
    send_packet((-2, 0), free_second)
    send_packet(north, free_lat)
    send_packet(south, free_lat)
    send_packet((0, 2), inner)
    send_packet((0, -2))
    send_blocks(east, lambda seen: near_cells(seen)[1:], even)
    send_blocks(east, lambda seen: near_cells(seen)[:1])
    send_blocks(east, lambda seen: near_cells(seen)[1:], odd)
    send_blocks(east, far_cells)
    for cells in (near_cells, far_cells):
        send_blocks(west, cells, free_west)
        send_blocks(north, cells, free_lat)
        send_blocks(south, cells, free_lat)
    wait_packet(west, rim)
    send_packet(west, rim)
    send_blocks(west, near_cells, rim)
    for block in (north, south):
        wait_packet(block, held_lat)
        send_packet(block, held_lat)
        serve(block, held_lat)
    for block in [(0, 2)] + west_side[1:]:
        wait_packet(block, rim)
        send_packet(block, rim)
    send_blocks(west, far_cells, rim)
    wait_packet((-2, 0), rim)
    send_packet((-2, 0), rim)

    cache = {}

    def field(name, cell):
        if (name, cell) in cache:
            return cache[name, cell]
        x, y = cell
        block = (x // 2, y // 2)
        p, r = x % 2, y % 2
        place = 2 * p + r
        if block in second_blocks:
            ref, at = PC, second_blocks.index(block)
            row = {"fe": 1 + r, "fn": 3 + p}.get(name, 0)
            assert (name != "fe" or p == 1) and (name != "fn" or r == 1)
        else:
            ref, at = PK, packet_blocks.index(block)
            row = {"fe": 8, "fn": 12, "vd": 16, "vc": 20}.get(name, 0) + place
        if name in ("land", "w"):
            lane_at = place + (4 if name == "w" else 0)
            row_values = ref[at, pl.ds(0, 1), :]
            value = jnp.broadcast_to(row_values[:, lane_at : lane_at + 1], (1, 128))
        else:
            value = ref[at, pl.ds(row, 1), :]
        cache[name, cell] = value
        return value

    def face(low, high):
        if ("face", low, high) not in cache:
            name = "fe" if low[1] == high[1] else "fn"
            cache["face", low, high] = field(name, low) * (field("land", low) * field("land", high))
        return cache["face", low, high]

    def between(cell, other):
        return face(*sorted((cell, other)))

    def coef(cell, row):
        return CF[pl.ds(COEFS * cell_index[cell] + row, 1), :]

    def edge(cell, other):
        return CF[pl.ds(edge_index[tuple(sorted((cell, other)))], 1), :]

    top = lax.broadcasted_iota(jnp.int32, (1, 128), 1) < 127

    def make_coefs(cell):
        x, y = cell
        p, r = x % 2, y % 2
        lon_cross, lon_same = ((x - 1, y), (x + 1, y)) if p == 0 else ((x + 1, y), (x - 1, y))
        lat_cross, lat_same = ((x, y - 1), (x, y + 1)) if r == 0 else ((x, y + 1), (x, y - 1))
        w = field("w", cell)
        vc = field("vc", cell)
        main = field("vd", cell) + vc + down(vc)
        for other in neighbours(cell):
            main = main + between(cell, other)
        same = between(cell, lon_same) * field("w", lon_same)
        same = same + between(cell, lat_same) * field("w", lat_same)
        weighted = w * main - same
        up = jnp.where(top, vc, 0.0)
        below = down(up)
        rows = [
            w,
            -relax * weighted,
            relax * w * below,
            relax * w * up,
            relax * between(cell, lon_cross) * field("w", lon_cross),
            relax * between(cell, lat_cross) * field("w", lat_cross),
        ]
        if cell in support:
            rows += [main, -below, -up]
        for row, values in enumerate(rows):
            CF[pl.ds(COEFS * cell_index[cell] + row, 1), :] = values

    def roll_down(values):
        return pltpu.roll(values, 1, 1)

    def roll_up(values):
        return pltpu.roll(values, 127, 1)

    diagonal = lax.broadcasted_iota(jnp.int32, (128, 128), 0) == lax.broadcasted_iota(
        jnp.int32, (128, 128), 1
    )

    def own_columns(cells):
        for cell in cells:
            inverse = block_value(cell)
            values = jnp.where(diagonal, coef(cell, 0), 0.0) + inverse * coef(cell, 1)
            values = values + roll_down(inverse) * coef(cell, 2) + roll_up(inverse) * coef(cell, 3)
            PT[cell_index[cell]] = values.T

    def near_columns(side):
        for cell in near_cells(side):
            inner = (cell[0] - side[0], cell[1] - side[1])
            scale = relax * between(cell, inner) * field("w", inner)
            PT[cell_index[cell]] = (block_value(cell) * scale).T

    def edges(early):
        for low, high in edge_list:
            if (high[0] >= 0 and low[0] >= 0) == early:
                CF[pl.ds(edge_index[low, high], 1), :] = face(low, high)

    filled = set()

    def add(block, values):
        place = slot_of[block]
        if place in filled:
            out[place] = out[place] + values
        else:
            out[place] = values
            filled.add(place)

    def galerkin(cell):
        x, y = cell
        a, b = x // 2, y // 2
        applied = None
        if cell in support:
            own = PT[cell_index[cell]]
            applied = own * coef(cell, 6) + roll_down(own) * coef(cell, 7) + roll_up(own) * coef(cell, 8)
        for other in neighbours(cell):
            if other in support:
                term = PT[cell_index[other]] * edge(cell, other)
                applied = -term if applied is None else applied - term
        high, low = split(applied)
        left = jnp.concatenate([high, low], axis=1)
        high, low = split(block_value(cell))
        right = jnp.concatenate([high, low], axis=1)
        right = jnp.concatenate([right, right], axis=0)
        product = jnp.dot(left, right, preferred_element_type=jnp.float32)
        product = product[:, :128] + product[:, 128:]
        own = applied * coef(cell, 0) + product * coef(cell, 1)
        own = own + roll_down(product) * coef(cell, 2) + roll_up(product) * coef(cell, 3)
        add((a, b), own)
        add((a + (1 if x % 2 else -1), b), product * coef(cell, 4))
        add((a, b + (1 if y % 2 else -1)), product * coef(cell, 5))

    def corner(block):
        landing = XC.at[corner_blocks.index(block)]
        wait(("corner", block), X.at[0, 0, 0], landing, (0, block[1]), exists(block))
        galerkin(corner_of(block))

    for block in (east, (2, 0), (1, 1), (1, -1), (0, -2)):
        wait_packet(block)
    wait_packet(north, free_lat)
    wait_packet(south, free_lat)
    wait_packet((0, 2), inner)
    for cell in all_cells:
        if cell[0] > 0:
            make_coefs(cell)
    edges(True)
    own_columns(own_cells[2:])
    pass_near(west, jnp.logical_not(late))
    for side in (east, north, south):
        pass_near(side)
        near_columns(side)
    for cell in near_cells(east):
        galerkin(cell)
    for side in (north, south):
        galerkin(near_cells(side)[1])
        for cell in far_cells(side):
            wait_block(cell)
        galerkin(far_cells(side)[1])
    for cell in far_cells(east):
        wait_block(cell)
        galerkin(cell)
    for block in corner_blocks:
        if block[0] > 0:
            corner(block)

    for block in west_side + [(-2, 0)]:
        wait_packet(block, inner)
        send_packet(block, phase <= 1 if block == (-2, 0) else late)
        if block == west:
            send_blocks(west, near_cells, late)
    for cell in all_cells:
        if cell[0] <= 0:
            make_coefs(cell)
    edges(False)
    own_columns(own_cells[:2])
    for cell in own_cells[2:]:
        galerkin(cell)
    for side in (north, south):
        for cell in (near_cells(side)[0], far_cells(side)[0]):
            galerkin(cell)
    pass_near(west, late)
    send_blocks(west, far_cells, late)
    near_columns(west)
    for cell in own_cells[:2] + near_cells(west):
        galerkin(cell)
    for block in corner_blocks:
        if block[0] < 0:
            corner(block)
    for cell in far_cells(west):
        wait_block(cell)
        galerkin(cell)
    assert len(filled) == len(offsets)
    for key, goal in sends:
        def drain(key=key, goal=goal):
            source = X.at[0, 0, 0]
            if key[0] == "packet":
                source = PK.at[0, pl.ds(0, 8)] if key[1] in second_blocks else PK.at[0]
            move(key, source, source, goal).wait_send()
        only(drains.get(key + (goal,), exists(goal)), drain)


def publish(held, out, sem):
    copies = [
        pltpu.make_async_copy(held.at[place], out.at[place], sem.at[place])
        for place in range(len(offsets))
    ]
    for copy in copies:
        copy.start()
    for copy in copies:
        copy.wait()


def local(inverse, vert_diag, vert_coup, face_east, face_north, land_mask, aggregate):
    blocks = len(offsets)
    messages = len(message)
    anywhere = pl.BlockSpec(memory_space=pltpu.HBM)
    held = pl.pallas_call(
        kernel,
        out_shape=pltpu.VMEM((blocks, 128, 128), jnp.float32),
        in_specs=[anywhere] * 7,
        out_specs=pl.BlockSpec(memory_space=pltpu.VMEM),
        scratch_shapes=[
            pltpu.VMEM((5, 2, 2, 128, 128), jnp.float32),
            pltpu.VMEM((4, 128, 128), jnp.float32),
            pltpu.VMEM((9, 24, 128), jnp.float32),
            pltpu.VMEM((4, 8, 128), jnp.float32),
            pltpu.VMEM((4, 2, 2, 128), jnp.float32),
            pltpu.VMEM((2, 2, 2), jnp.int32),
            pltpu.VMEM((len(support), 128, 128), jnp.float32),
            pltpu.VMEM((coef_rows, 128), jnp.float32),
            pltpu.SemaphoreType.DMA((7,)),
            pltpu.SemaphoreType.DMA((messages,)),
            pltpu.SemaphoreType.DMA((messages,)),
        ],
        compiler_params=pltpu.CompilerParams(collective_id=0, has_side_effects=True),
    )(inverse, vert_diag, vert_coup, face_east, face_north, land_mask, aggregate)
    coarse = pl.pallas_call(
        publish,
        out_shape=jax.ShapeDtypeStruct((blocks, 128, 128), jnp.float32),
        in_specs=[pl.BlockSpec(memory_space=pltpu.VMEM)],
        out_specs=anywhere,
        scratch_shapes=[pltpu.SemaphoreType.DMA((blocks,))],
        compiler_params=pltpu.CompilerParams(vmem_limit_bytes=2**20),
    )(held)
    return coarse[None, None]


def solution(mesh):
    return jax.shard_map(
        local,
        mesh=mesh,
        in_specs=(
            P("lon", "lat", None, None),
            P("lon", "lat", None),
            P("lon", "lat", None),
            P("lon", "lat", None),
            P("lon", "lat", None),
            P("lon", "lat"),
            P("lon", "lat"),
        ),
        out_specs=P("lon", "lat", None, None, None),
        check_vma=False,
    )
```

```python
import jax
import jax.numpy as jnp
from jax import lax
from jax.experimental import pallas as pl
from jax.experimental.pallas import tpu as pltpu
from jax.sharding import PartitionSpec as P

MESH = pl.DeviceIdType.MESH
relax = 0.6
offsets = [
    (-2, 0),
    (-1, -1),
    (-1, 0),
    (-1, 1),
    (0, -2),
    (0, -1),
    (0, 0),
    (0, 1),
    (0, 2),
    (1, -1),
    (1, 0),
    (1, 1),
    (2, 0),
]
slot_of = {offset: place for place, offset in enumerate(offsets)}
near_blocks = [(0, 0), (1, 0), (-1, 0), (0, 1), (0, -1)]
second_blocks = [(2, 0), (-2, 0), (0, 2), (0, -2)]
corner_blocks = [(1, 1), (-1, 1), (1, -1), (-1, -1)]
packet_blocks = near_blocks + corner_blocks
sides = [(1, 0), (-1, 0), (0, 1), (0, -1)]


def corner_cell(block):
    return (0 if block[0] > 0 else 1, 0 if block[1] > 0 else 1)


def cells_of(block):
    return [(2 * block[0] + p, 2 * block[1] + r) for p in (0, 1) for r in (0, 1)]


def near_cells(side):
    a, b = side
    if b == 0:
        p = 0 if a > 0 else 1
        return [(2 * a + p, r) for r in (0, 1)]
    r = 0 if b > 0 else 1
    return [(p, 2 * b + r) for p in (0, 1)]


def far_cells(side):
    near = near_cells(side)
    return [cell for cell in cells_of(side) if cell not in near]


def neighbours(cell):
    x, y = cell
    return [(x + 1, y), (x - 1, y), (x, y + 1), (x, y - 1)]


own_cells = cells_of((0, 0))
support = own_cells + [cell for side in sides for cell in near_cells(side)]
outer = [cell for side in sides for cell in far_cells(side)] + [
    (2 * a + corner_cell((a, b))[0], 2 * b + corner_cell((a, b))[1]) for a, b in corner_blocks
]
all_cells = support + outer
cell_index = {cell: place for place, cell in enumerate(all_cells)}
COEFS = 9
edge_list = []
for cell in support:
    for other in neighbours(cell):
        key = tuple(sorted((cell, other)))
        if key not in edge_list:
            edge_list.append(key)
edge_index = {edge: COEFS * len(all_cells) + place for place, edge in enumerate(edge_list)}
coef_rows = COEFS * len(all_cells) + len(edge_list)
coef_rows = (coef_rows + 7) // 8 * 8

message = {}
for block in near_blocks[1:] + second_blocks + corner_blocks:
    message["packet", block] = len(message)
for side in sides:
    for cell in near_cells(side) + far_cells(side):
        message["block", cell] = len(message)
for block in corner_blocks:
    message["corner", block] = len(message)


def down(values):
    lane = lax.broadcasted_iota(jnp.int32, values.shape, 1)
    return jnp.where(lane > 0, pltpu.roll(values, 1, 1), 0.0)


def split(values):
    high = values.astype(jnp.bfloat16)
    low = (values - high.astype(jnp.float32)).astype(jnp.bfloat16)
    return high, low


def kernel(
    inv_h, vd_h, vc_h, fe_h, fn_h, land_h, agg_h,
    out,
    X, XC, PK, PC, SM, LA, PT, CF,
    local_sem, send_sem, recv_sem, ready,
):
    me_lon = lax.axis_index("lon")
    me_lat = lax.axis_index("lat")
    count_lon = lax.axis_size("lon")
    count_lat = lax.axis_size("lat")
    own_of = {"vd": 0, "vc": 1, "fe": 2, "fn": 3}
    east, west, north, south = sides

    small_copies = [
        pltpu.make_async_copy(source, SM.at[place], local_sem.at[1 + place])
        for place, source in enumerate((vd_h, vc_h, fe_h, fn_h))
    ] + [
        pltpu.make_async_copy(source, LA.at[place], local_sem.at[5 + place])
        for place, source in enumerate((land_h, agg_h))
    ]
    inverse_copy = pltpu.make_async_copy(inv_h, X.at[0], local_sem.at[0])
    for copy in small_copies:
        copy.start()
    inverse_copy.start()

    def target(block):
        a, b = block
        return {"lon": lax.rem(me_lon + a + count_lon, count_lon), "lat": me_lat + b}

    inside = {b: me_lat + b < count_lat if b > 0 else me_lat + b >= 0 for b in (-2, -1, 1, 2)}

    def exists(block):
        return inside.get(block[1])

    def both(first, second):
        if first is None:
            return second
        return first if second is None else jnp.logical_and(first, second)

    def only(condition, action):
        if condition is None:
            action()
        else:
            pl.when(condition)(action)

    phase = lax.rem(me_lon, 64)
    late = phase == 0
    rim = phase == 63
    inner = phase < 63
    even = lax.rem(me_lat, 2) == 0
    odd = lax.rem(me_lat, 2) == 1
    across_up = jnp.logical_and(odd, me_lat + 1 < count_lat)
    across_down = jnp.logical_and(even, me_lat >= 1)
    barrier = pltpu.get_barrier_semaphore()
    for block in near_blocks[1:] + second_blocks + corner_blocks:
        reach = None
        if block[0] > 0:
            reach = phase < 63 - block[0]
        elif block == (0, 1):
            reach = jnp.logical_or(inner, odd)
        elif block == (0, -1):
            reach = jnp.logical_or(inner, odd)
        elif block == (0, -2):
            reach = inner
        def signal(block=block):
            pl.semaphore_signal(barrier, inc=1, device_id=target(block), device_id_type=MESH)
        only(both(exists(block), reach), signal)

    partners = near_blocks[1:] + second_blocks + corner_blocks
    for block in partners:
        if block[1] == 0:
            continue
        def clear(block=block):
            if block in second_blocks:
                PC[second_blocks.index(block)] = jnp.zeros((8, 128), jnp.float32)
                return
            PK[packet_blocks.index(block)] = jnp.zeros((24, 128), jnp.float32)
            if block in near_blocks:
                X[near_blocks.index(block)] = jnp.zeros((2, 2, 128, 128), jnp.float32)
            else:
                XC[corner_blocks.index(block)] = jnp.zeros((128, 128), jnp.float32)
        pl.when(jnp.logical_not(exists(block)))(clear)

    lat_near = jnp.where(inside[1], 1, 0) + jnp.where(inside[-1], 1, 0)
    lat_second = jnp.where(inside[2], 1, 0) + jnp.where(inside[-2], 1, 0)
    from_west = jnp.where(late, 0, 1 + lat_near) + jnp.where(phase > 1, 1, 0)
    awaited_inner = lat_near + lat_second + from_west
    awaited_rim = jnp.where(even, lat_near, 0) + jnp.where(inside[-2], 1, 0)
    pl.semaphore_wait(barrier, 2 + lat_near + jnp.where(rim, awaited_rim, awaited_inner))

    @pl.when(rim)
    def _():
        pl.semaphore_signal(ready, inc=1, device_id=target(east), device_id_type=MESH)

    for copy in small_copies:
        copy.wait()
    live = (LA[1] >= 0).astype(jnp.float32)
    land = LA[0].astype(jnp.float32)

    def spread(values, p, r):
        return jnp.broadcast_to(values[p : p + 1, r : r + 1], (1, 128))

    lives = {(p, r): spread(live, p, r) for p in (0, 1) for r in (0, 1)}
    block_count = lives[0, 0] + lives[0, 1] + lives[1, 0] + lives[1, 1]
    norm = jnp.sqrt(jnp.maximum(block_count, 1.0))
    lane = lax.broadcasted_iota(jnp.int32, (1, 128), 1)
    scalars = jnp.zeros((1, 128), jnp.float32)
    for p in (0, 1):
        for r in (0, 1):
            scalars = jnp.where(lane == 2 * p + r, spread(land, p, r), scalars)
            scalars = jnp.where(lane == 4 + 2 * p + r, lives[p, r] / norm, scalars)

    def mine(field, p, r):
        return SM[own_of[field], p, pl.ds(r, 1), :]

    blank = jnp.zeros((1, 128), jnp.float32)
    head = [scalars, mine("fe", 1, 0), mine("fe", 1, 1), mine("fn", 0, 1), mine("fn", 1, 1)]
    for row, values in enumerate(head + [blank] * 3):
        PK[0, pl.ds(row, 1), :] = values
    for first, field in ((8, "fe"), (12, "fn"), (16, "vd"), (20, "vc")):
        for p in (0, 1):
            for r in (0, 1):
                PK[0, pl.ds(first + 2 * p + r, 1), :] = mine(field, p, r)

    sends = []

    def move(key, source, landing, block):
        place = message[key]
        return pltpu.make_async_remote_copy(
            src_ref=source,
            dst_ref=landing,
            send_sem=send_sem.at[place],
            recv_sem=recv_sem.at[place],
            device_id=target(block),
            device_id_type=MESH,
        )

    def opposite(block):
        return (-block[0], -block[1])

    def packet_ref(block):
        if block in second_blocks:
            return PC.at[second_blocks.index(block)]
        return PK.at[packet_blocks.index(block)]

    def block_ref(cell):
        x, y = cell
        block = (x // 2, y // 2)
        if block in near_blocks:
            return X.at[near_blocks.index(block), x % 2, y % 2]
        return XC.at[corner_blocks.index(block)]

    def block_value(cell):
        x, y = cell
        block = (x // 2, y // 2)
        if block in near_blocks:
            return X[near_blocks.index(block), x % 2, y % 2]
        return XC[corner_blocks.index(block)]

    def corner_of(block):
        p, r = corner_cell(block)
        return (2 * block[0] + p, 2 * block[1] + r)

    listed = set()
    drains = {}

    def send(key, source, landing, goal, condition):
        copy = move(key, source, landing, goal)
        only(condition, copy.start)
        if (key, goal) not in listed:
            sends.append((key, goal))
            listed.add((key, goal))

    def send_packet(goal, condition=None):
        seen = opposite(goal)
        source = PK.at[0, pl.ds(0, 8)] if seen in second_blocks else PK.at[0]
        send(("packet", seen), source, packet_ref(seen), goal, both(exists(goal), condition))

    def send_blocks(goal, cells, condition=None):
        seen = opposite(goal)
        for cell in cells(seen):
            source = X.at[0, cell[0] % 2, cell[1] % 2]
            send(("block", cell), source, block_ref(cell), goal, both(exists(goal), condition))

    def pass_block(side, cell, condition):
        wait_block(cell, condition)
        if side not in (east, west):
            return
        goal = north if cell[1] else south
        seen = (side[0], -goal[1])
        landing = block_ref(corner_of(seen))
        facing = exists(goal)
        if side == west:
            facing = even if goal == north else odd
        send(("corner", seen), block_ref(cell), landing, goal, both(facing, condition))
        drains["corner", seen, goal] = facing

    def pass_near(side, condition=None):
        first, second = near_cells(side)
        if side == west:
            pass_block(side, second, both(condition, even))
            pass_block(side, first, condition)
            pass_block(side, second, both(condition, odd))
        else:
            pass_block(side, first, condition)
            pass_block(side, second, condition)

    def send_across(goal, condition):
        seen = opposite(goal)
        cell = corner_of(seen)
        source = X.at[0, cell[0] % 2, cell[1] % 2]
        send(("corner", seen), source, block_ref(cell), goal, condition)
        drains["corner", seen, goal] = condition

    def wait(key, source, landing, origin, condition):
        only(condition, move(key, source, landing, origin).wait_recv)

    def wait_packet(block, condition=None):
        landing = packet_ref(block)
        source = PK.at[0, pl.ds(0, 8)] if block in second_blocks else PK.at[0]
        wait(("packet", block), source, landing, block, both(exists(block), condition))

    def wait_block(cell, condition=None):
        block = (cell[0] // 2, cell[1] // 2)
        arrived = both(exists(block), condition)
        wait(("block", cell), X.at[0, 0, 0], block_ref(cell), block, arrived)

    def serve(goal, condition=None):
        for cells in (near_cells, far_cells):
            send_blocks(goal, cells, condition)

    west_side = [west, (-1, 1), (-1, -1)]
    free_west = jnp.logical_and(phase > 0, inner)
    free_second = jnp.logical_and(phase > 1, inner)
    held_lat = jnp.logical_and(rim, odd)
    free_lat = jnp.logical_not(held_lat)
    for goal in (east, (2, 0), (1, 1), (1, -1)):
        send_packet(goal)
    inverse_copy.wait()
    send_across((1, 1), across_up)
    send_across((1, -1), across_down)
    for goal in west_side:
        send_packet(goal, free_west)
    send_packet((-2, 0), free_second)
    send_packet(north, free_lat)
    send_packet(south, free_lat)
    send_packet((0, 2), inner)
    send_packet((0, -2))
    send_blocks(east, lambda seen: near_cells(seen)[1:], even)
    send_blocks(east, lambda seen: near_cells(seen)[:1])
    send_blocks(east, lambda seen: near_cells(seen)[1:], odd)
    send_blocks(east, far_cells)
    for cells in (near_cells, far_cells):
        send_blocks(west, cells, free_west)
        send_blocks(north, cells, free_lat)
        send_blocks(south, cells, free_lat)
    wait_packet(west, rim)
    send_packet(west, rim)
    send_blocks(west, near_cells, rim)
    for block in (north, south):
        wait_packet(block, held_lat)
        send_packet(block, held_lat)
        serve(block, held_lat)
    for block in [(0, 2)] + west_side[1:]:
        wait_packet(block, rim)
        send_packet(block, rim)
    send_blocks(west, far_cells, rim)
    wait_packet((-2, 0), rim)
    send_packet((-2, 0), rim)

    cache = {}

    def field(name, cell):
        if (name, cell) in cache:
            return cache[name, cell]
        x, y = cell
        block = (x // 2, y // 2)
        p, r = x % 2, y % 2
        place = 2 * p + r
        if block in second_blocks:
            ref, at = PC, second_blocks.index(block)
            row = {"fe": 1 + r, "fn": 3 + p}.get(name, 0)
            assert (name != "fe" or p == 1) and (name != "fn" or r == 1)
        else:
            ref, at = PK, packet_blocks.index(block)
            row = {"fe": 8, "fn": 12, "vd": 16, "vc": 20}.get(name, 0) + place
        if name in ("land", "w"):
            lane_at = place + (4 if name == "w" else 0)
            row_values = ref[at, pl.ds(0, 1), :]
            value = jnp.broadcast_to(row_values[:, lane_at : lane_at + 1], (1, 128))
        else:
            value = ref[at, pl.ds(row, 1), :]
        cache[name, cell] = value
        return value

    def face(low, high):
        if ("face", low, high) not in cache:
            name = "fe" if low[1] == high[1] else "fn"
            cache["face", low, high] = field(name, low) * (field("land", low) * field("land", high))
        return cache["face", low, high]

    def between(cell, other):
        return face(*sorted((cell, other)))

    def coef(cell, row):
        return CF[pl.ds(COEFS * cell_index[cell] + row, 1), :]

    def edge(cell, other):
        return CF[pl.ds(edge_index[tuple(sorted((cell, other)))], 1), :]

    top = lax.broadcasted_iota(jnp.int32, (1, 128), 1) < 127

    def make_coefs(cell):
        x, y = cell
        p, r = x % 2, y % 2
        lon_cross, lon_same = ((x - 1, y), (x + 1, y)) if p == 0 else ((x + 1, y), (x - 1, y))
        lat_cross, lat_same = ((x, y - 1), (x, y + 1)) if r == 0 else ((x, y + 1), (x, y - 1))
        w = field("w", cell)
        vc = field("vc", cell)
        main = field("vd", cell) + vc + down(vc)
        for other in neighbours(cell):
            main = main + between(cell, other)
        same = between(cell, lon_same) * field("w", lon_same)
        same = same + between(cell, lat_same) * field("w", lat_same)
        weighted = w * main - same
        up = jnp.where(top, vc, 0.0)
        below = down(up)
        rows = [
            w,
            -relax * weighted,
            relax * w * below,
            relax * w * up,
            relax * between(cell, lon_cross) * field("w", lon_cross),
            relax * between(cell, lat_cross) * field("w", lat_cross),
        ]
        if cell in support:
            rows += [main, -below, -up]
        for row, values in enumerate(rows):
            CF[pl.ds(COEFS * cell_index[cell] + row, 1), :] = values

    def roll_down(values):
        return pltpu.roll(values, 1, 1)

    def roll_up(values):
        return pltpu.roll(values, 127, 1)

    diagonal = lax.broadcasted_iota(jnp.int32, (128, 128), 0) == lax.broadcasted_iota(
        jnp.int32, (128, 128), 1
    )

    def own_columns(cells):
        for cell in cells:
            inverse = block_value(cell)
            values = jnp.where(diagonal, coef(cell, 0), 0.0) + inverse * coef(cell, 1)
            values = values + roll_down(inverse) * coef(cell, 2) + roll_up(inverse) * coef(cell, 3)
            PT[cell_index[cell]] = values.T

    def near_columns(side):
        for cell in near_cells(side):
            inner = (cell[0] - side[0], cell[1] - side[1])
            scale = relax * between(cell, inner) * field("w", inner)
            PT[cell_index[cell]] = (block_value(cell) * scale).T

    def edges(early):
        for low, high in edge_list:
            if (high[0] >= 0 and low[0] >= 0) == early:
                CF[pl.ds(edge_index[low, high], 1), :] = face(low, high)

    filled = set()

    def add(block, values):
        place = slot_of[block]
        if place in filled:
            out[place] = out[place] + values
        else:
            out[place] = values
            filled.add(place)

    def galerkin(cell):
        x, y = cell
        a, b = x // 2, y // 2
        applied = None
        if cell in support:
            own = PT[cell_index[cell]]
            applied = own * coef(cell, 6) + roll_down(own) * coef(cell, 7) + roll_up(own) * coef(cell, 8)
        for other in neighbours(cell):
            if other in support:
                term = PT[cell_index[other]] * edge(cell, other)
                applied = -term if applied is None else applied - term
        high, low = split(applied)
        left = jnp.concatenate([high, low], axis=1)
        high, low = split(block_value(cell))
        right = jnp.concatenate([high, low], axis=1)
        right = jnp.concatenate([right, right], axis=0)
        product = jnp.dot(left, right, preferred_element_type=jnp.float32)
        product = product[:, :128] + product[:, 128:]
        own = applied * coef(cell, 0) + product * coef(cell, 1)
        own = own + roll_down(product) * coef(cell, 2) + roll_up(product) * coef(cell, 3)
        add((a, b), own)
        add((a + (1 if x % 2 else -1), b), product * coef(cell, 4))
        add((a, b + (1 if y % 2 else -1)), product * coef(cell, 5))

    def corner(block):
        landing = XC.at[corner_blocks.index(block)]
        wait(("corner", block), X.at[0, 0, 0], landing, (0, block[1]), exists(block))
        galerkin(corner_of(block))

    for block in (east, (2, 0), (1, 1), (1, -1), (0, -2)):
        wait_packet(block)
    wait_packet(north, free_lat)
    wait_packet(south, free_lat)
    wait_packet((0, 2), inner)
    for cell in all_cells:
        if cell[0] > 0:
            make_coefs(cell)
    edges(True)
    own_columns(own_cells[2:])
    pass_near(west, jnp.logical_not(late))
    for side in (east, north, south):
        pass_near(side)
        near_columns(side)
    for cell in near_cells(east):
        galerkin(cell)
    for side in (north, south):
        galerkin(near_cells(side)[1])
        for cell in far_cells(side):
            wait_block(cell)
        galerkin(far_cells(side)[1])
    for cell in far_cells(east):
        wait_block(cell)
        galerkin(cell)
    for block in corner_blocks:
        if block[0] > 0:
            corner(block)

    @pl.when(late)
    def _():
        pl.semaphore_wait(ready, 1)

    send_blocks(west, near_cells, late)
    for block in west_side + [(-2, 0)]:
        wait_packet(block, inner)
        send_packet(block, phase <= 1 if block == (-2, 0) else late)
    for cell in all_cells:
        if cell[0] <= 0:
            make_coefs(cell)
    edges(False)
    own_columns(own_cells[:2])
    for cell in own_cells[2:]:
        galerkin(cell)
    for side in (north, south):
        for cell in (near_cells(side)[0], far_cells(side)[0]):
            galerkin(cell)
    pass_near(west, late)
    send_blocks(west, far_cells, late)
    near_columns(west)
    for cell in own_cells[:2] + near_cells(west):
        galerkin(cell)
    for block in corner_blocks:
        if block[0] < 0:
            corner(block)
    for cell in far_cells(west):
        wait_block(cell)
        galerkin(cell)
    assert len(filled) == len(offsets)
    for key, goal in sends:
        def drain(key=key, goal=goal):
            source = X.at[0, 0, 0]
            if key[0] == "packet":
                source = PK.at[0, pl.ds(0, 8)] if key[1] in second_blocks else PK.at[0]
            move(key, source, source, goal).wait_send()
        only(drains.get(key + (goal,), exists(goal)), drain)


def publish(held, out, sem):
    copies = [
        pltpu.make_async_copy(held.at[place], out.at[place], sem.at[place])
        for place in range(len(offsets))
    ]
    for copy in copies:
        copy.start()
    for copy in copies:
        copy.wait()


def local(inverse, vert_diag, vert_coup, face_east, face_north, land_mask, aggregate):
    blocks = len(offsets)
    messages = len(message)
    anywhere = pl.BlockSpec(memory_space=pltpu.HBM)
    held = pl.pallas_call(
        kernel,
        out_shape=pltpu.VMEM((blocks, 128, 128), jnp.float32),
        in_specs=[anywhere] * 7,
        out_specs=pl.BlockSpec(memory_space=pltpu.VMEM),
        scratch_shapes=[
            pltpu.VMEM((5, 2, 2, 128, 128), jnp.float32),
            pltpu.VMEM((4, 128, 128), jnp.float32),
            pltpu.VMEM((9, 24, 128), jnp.float32),
            pltpu.VMEM((4, 8, 128), jnp.float32),
            pltpu.VMEM((4, 2, 2, 128), jnp.float32),
            pltpu.VMEM((2, 2, 2), jnp.int32),
            pltpu.VMEM((len(support), 128, 128), jnp.float32),
            pltpu.VMEM((coef_rows, 128), jnp.float32),
            pltpu.SemaphoreType.DMA((7,)),
            pltpu.SemaphoreType.DMA((messages,)),
            pltpu.SemaphoreType.DMA((messages,)),
            pltpu.SemaphoreType.REGULAR,
        ],
        compiler_params=pltpu.CompilerParams(collective_id=0, has_side_effects=True),
    )(inverse, vert_diag, vert_coup, face_east, face_north, land_mask, aggregate)
    coarse = pl.pallas_call(
        publish,
        out_shape=jax.ShapeDtypeStruct((blocks, 128, 128), jnp.float32),
        in_specs=[pl.BlockSpec(memory_space=pltpu.VMEM)],
        out_specs=anywhere,
        scratch_shapes=[pltpu.SemaphoreType.DMA((blocks,))],
        compiler_params=pltpu.CompilerParams(vmem_limit_bytes=2**20),
    )(held)
    return coarse[None, None]


def solution(mesh):
    return jax.shard_map(
        local,
        mesh=mesh,
        in_specs=(
            P("lon", "lat", None, None),
            P("lon", "lat", None),
            P("lon", "lat", None),
            P("lon", "lat", None),
            P("lon", "lat", None),
            P("lon", "lat"),
            P("lon", "lat"),
        ),
        out_specs=P("lon", "lat", None, None, None),
        check_vma=False,
    )
```
